32 devices in a mesh: tm: 4 (over x, core), env: 8 (over z, y).
Axes of the slice: x: 2, y: 2, z: 4, core: 2. Of those that a mesh axis runs over, the one named last changes fastest.
Arguments:
- rewards: float32 [2048, 4096], P('tm', 'env'), may hold values from -0.4 to 0.4
- values: float32 [2048, 4096], P('tm', 'env'), may hold values from -0.4 to 0.4
- done_flags: int32 [2048, 4096], P('tm', 'env'), may hold values 0 or 1
- bootstrap: float32 [4096], P('env'), may hold values from -0.4 to 0.4
- discount_horizon: float32 [4096], P('env'), may hold values from 10 to 16384
- trace_horizon: float32 [4096], P('env'), may hold values from 10 to 16384
Outputs:
- norm_advantage: float32 [2048, 4096], P('tm', 'env')
- return_target: float32 [2048, 4096], P('tm', 'env')
The draws below stay inside these ranges and needn't reach their ends.
All inputs are finite; a program needn't handle non-finite values. No bound on the sum of `done_flags` on one device may be relied on, other than what follows from the above.
Results may differ from the reference program's by a relative error of at most 0.0003.
Values sent between devices are 32-bit elements; how exact they have to be, the bound alone decides.
A program may use at most 64 MiB of HBM per device.

```python
import jax
import jax.numpy as jnp
from jax import lax

STEPS = 2048
ENVS = 4096


def short_flags(key):
    flag_key = jax.random.fold_in(key, 5)
    share_key, pick_key = jax.random.split(flag_key)
    share_short = jax.random.uniform(share_key, (), jnp.float32, 0.35, 0.65)
    return jax.random.uniform(pick_key, (ENVS,), jnp.float32) < share_short


def horizon_values(key, salt):
    flags = short_flags(key)
    own_key = jax.random.fold_in(key, salt)
    short_key, long_key = jax.random.split(own_key)
    short_value = jnp.exp(jax.random.uniform(short_key, (ENVS,), jnp.float32, jnp.log(10.0), jnp.log(40.0)))
    long_value = jnp.exp(jax.random.uniform(long_key, (ENVS,), jnp.float32, jnp.log(2.0 * STEPS), jnp.log(8.0 * STEPS)))
    picked = jnp.where(flags, short_value, long_value)
    return jnp.clip(picked, 10.0, 8.0 * STEPS).astype(jnp.float32)


def draw_discount_horizon(key, part):
    return horizon_values(key, 11)


def draw_trace_horizon(key, part):
    return horizon_values(key, 23)


def plant(result, rng, smallest, largest):
    dims = result.shape
    index_at = [jax.random.randint(jax.random.fold_in(rng, axis), (), 0, dims[axis]) for axis in range(len(dims))]
    result = result.at[tuple(index_at)].set(smallest)
    longest = dims.index(max(dims))
    index_at[longest] = (index_at[longest] + 1) % dims[longest]
    return result.at[tuple(index_at)].set(largest)


def block_levels(key, dims, pieces, low, top_value):
    level, own = 1.0, jax.random.fold_in(key, 6)
    for axis_at, parts in pieces:
        heights = jnp.exp(jax.random.uniform(jax.random.fold_in(own, axis_at), (parts,), jnp.float32, low / len(pieces), top_value / len(pieces)))
        level = level * jnp.repeat(heights, dims[axis_at] // parts).reshape([-1 if axis == axis_at else 1 for axis in range(len(dims))])
    return level


def gaussian(rng, dims, spread, most, shards=(), dtype=jnp.bfloat16):
    loudness = block_levels(rng, dims, shards, -0.22, 0.18) if shards else 1.0
    drawn = jax.random.normal(rng, dims, jnp.float32) * spread * loudness
    return jnp.minimum(jnp.maximum(drawn, -most), most).astype(dtype)


def setup_inputs(seed: int = 0) -> dict:
    seeds = jax.random.split(jax.random.key(seed), 7)
    return {
        "rewards": gaussian(seeds[0], (STEPS, ENVS), 0.05, 0.4, ((0, 4), (1, 8)), jnp.float32),
        "values": gaussian(seeds[1], (STEPS, ENVS), 0.05, 0.4, ((0, 4), (1, 8)), jnp.float32),
        "done_flags": plant((jax.random.randint(seeds[2], (STEPS, ENVS), 0, 2 * STEPS) < 1).astype(jnp.int32), jax.random.fold_in(seeds[2], 1), 0, 1),
        "bootstrap": gaussian(seeds[3], (ENVS,), 0.05, 0.4, ((0, 8),), jnp.float32),
        "discount_horizon": draw_discount_horizon(jax.random.fold_in(seeds[6], 71), 0),
        "trace_horizon": draw_trace_horizon(jax.random.fold_in(seeds[6], 71), 0),
    }


def reference(rewards, values, done_flags, bootstrap, discount_horizon, trace_horizon):
    discount = 1.0 - 1.0 / discount_horizon
    trace_decay = 1.0 - 1.0 / trace_horizon
    keep_mask = 1.0 - done_flags.astype(jnp.float32)
    next_value = jnp.concatenate([values[1:], bootstrap[None, :]], axis=0)
    step_error = rewards + discount[None, :] * next_value * keep_mask - values
    carry_rate = (discount * trace_decay)[None, :] * keep_mask

    def stepper(carry_in, row):
        rate_row, error_row = row
        gain_row = error_row + rate_row * carry_in
        return (gain_row, gain_row)
    start_carry = jnp.zeros_like(bootstrap)
    _, advantage = lax.scan(stepper, start_carry, (carry_rate, step_error), reverse=True)
    cell_count = 1.0 * advantage.size
    mean_value = jnp.sum(advantage) / cell_count
    variance = jnp.sum((advantage - mean_value) ** 2) / cell_count
    norm_advantage = (advantage - mean_value) / jnp.sqrt(variance + 1.0)
    return_target = advantage + values
    return (norm_advantage, return_target)
```

```python
import functools

import jax
import jax.numpy as jnp
from jax import lax
from jax.experimental import pallas as pl
from jax.experimental.pallas import tpu as pltpu
from jax.sharding import PartitionSpec as P

MESH = pl.DeviceIdType.MESH
SEGMENTS = 8
LANES = 128
PAD = 8
STEPS_UNROLLED = 16
VMEM_BYTES = 67043328
SUMS = 5
ROWS = 7
scope = jax.named_scope


def shifted(x, distance, fill):
    rows = lax.broadcasted_iota(jnp.int32, x.shape, 0)
    moved = pltpu.roll(x, SEGMENTS - distance, 0)
    return jnp.where(rows < SEGMENTS - distance, moved, fill)


def send_groups(chunks):
    return ((0, chunks - 1), (chunks - 1, 1)) if chunks > 1 else ((0, 1),)


def exchange_kernel(
    num_tm, num_env, cells,
    rewards_hbm, values_hbm, flags_hbm, boot_hbm, disc_hbm, trace_hbm,
    adv_ref, ret_ref, stats_ref,
    rew, val, flg, params, base, prop, out, links, table, news,
    param_sem, load_sem, send_sem, link_sem, root_sem, news_sem,
):
    me = lax.axis_index("tm")
    my_env = lax.axis_index("env")
    seg_rows, width = rewards_hbm.shape[1], rewards_hbm.shape[2]
    chunks = width // LANES
    pitch = seg_rows + PAD
    groups = send_groups(chunks)
    last = chunks - 1
    root_tm = 1 if num_tm % 2 == 0 else 0
    is_root = jnp.logical_and(me == root_tm, my_env == 0)
    others = num_tm * num_env - 1

    def rows_of(ref, n):
        count = 1
        for d in ref.shape[:-1]:
            count *= d
        return ref.reshape(count, LANES).at[pl.ds(0, n)]

    def pending(sem, n, ref=base):
        part = rows_of(ref, n)
        return pltpu.make_async_remote_copy(
            src_ref=part, dst_ref=part, send_sem=sem, recv_sem=sem,
            device_id={"tm": lax.rem(me + 1, num_tm)}, device_id_type=MESH,
        )

    def load(j):
        for s in range(SEGMENTS):
            for hbm, vmem in ((rewards_hbm, rew), (values_hbm, val), (flags_hbm, flg)):
                pltpu.make_async_copy(
                    hbm.at[s, :, pl.ds(j * LANES, LANES)], vmem.at[j, :, s], load_sem.at[j]
                ).start()

    load(0)
    for a, hbm in enumerate((boot_hbm, disc_hbm, trace_hbm)):
        pltpu.make_async_copy(hbm, params.at[a], param_sem.at[0]).start()
    for j in range(1, chunks):
        load(j)

    barrier = pltpu.get_barrier_semaphore()
    for k in range(1, num_tm):
        pl.semaphore_signal(barrier, inc=1, device_id={"tm": lax.rem(me + k, num_tm)}, device_id_type=MESH)

    @pl.when(my_env != 0)
    def _():
        pl.semaphore_signal(barrier, inc=1, device_id={"tm": root_tm, "env": 0}, device_id_type=MESH)

    @pl.when(is_root)
    def _():
        def greet(e, state):
            for t in range(num_tm):
                pl.semaphore_signal(barrier, inc=1, device_id={"tm": t, "env": e}, device_id_type=MESH)
            return state

        lax.fori_loop(1, num_env, greet, 0)

    def link_copy(peer, g):
        first, count = groups[g]
        return pltpu.make_async_remote_copy(
            src_ref=out.at[pl.ds(first, count), pl.ds(0, 2)], dst_ref=links.at[me, pl.ds(first, count), pl.ds(0, 2)],
            send_sem=send_sem.at[0], recv_sem=link_sem.at[0],
            device_id={"tm": peer}, device_id_type=MESH,
        )

    def root_copy(g):
        first, count = groups[g]
        rows = ROWS if first + count == chunks else SUMS
        return pltpu.make_async_remote_copy(
            src_ref=out.at[pl.ds(first, count), pl.ds(0, rows)],
            dst_ref=table.at[me, pl.ds(first, count), pl.ds(0, rows), my_env],
            send_sem=send_sem.at[0], recv_sem=root_sem.at[g],
            device_id={"tm": root_tm, "env": 0}, device_id_type=MESH,
        )

    sent_rows = [count * SUMS + (ROWS - SUMS if first + count == chunks else 0) for first, count in groups]
    peers = [lax.rem(me + k, num_tm) for k in range(1, num_tm)]

    with scope("parw"):
        pending(param_sem.at[0], 3 * chunks).wait_recv()
    inv_trace = 1.0 / (1.0 - 1.0 / params[2])
    discount = 1.0 - 1.0 / params[1]
    rate_all = discount * (1.0 - 1.0 / params[2])
    top = me == num_tm - 1
    ends = jnp.where(top, params[0] * inv_trace, 0.0)
    open_end = jnp.where(top, 0.0, 1.0)

    own = []
    zero = jnp.zeros((SEGMENTS, LANES), jnp.float32)
    total, squares = zero, zero
    for j in range(chunks):
        spread = lambda x: jnp.broadcast_to(x[:, j * LANES:(j + 1) * LANES], zero.shape)
        disc, rate, itr, end = spread(discount), spread(rate_all), spread(inv_trace), spread(ends)

        def steps(i, state, j=j, disc=disc, rate=rate):
            b, p, nv, s1, s2, s3, s4, s5 = state
            for u in range(STEPS_UNROLLED):
                r = seg_rows - 1 - (i * STEPS_UNROLLED + u)
                v = val[j, r]
                live = flg[j, r] == 0
                d = jnp.where(live, disc, 0.0)
                g = jnp.where(live, rate, 0.0)
                b = (rew[j, r] - v + d * nv) + g * b
                p = g * p
                nv = v
                base[j, r] = b
                prop[j, r] = p
                s1, s2, s3, s4, s5 = s1 + b, s2 + p, s3 + b * b, s4 + b * p, s5 + p * p
            return b, p, nv, s1, s2, s3, s4, s5

        with scope(f"ldw{j}"):
            pending(load_sem.at[j], 3 * seg_rows * SEGMENTS).wait_recv()
        with scope(f"scan{j}"):
            state = lax.fori_loop(0, seg_rows // STEPS_UNROLLED, steps, (zero, zero + 1.0, zero) + (zero,) * 5)
        b, p, v, s1, s2, s3, s4, s5 = state
        x, a = b + v * itr, p
        for d in (1, 2, 4):
            x_next, a_next = shifted(x, d, 0.0), shifted(a, d, 1.0)
            x, a = x + a * x_next, a * a_next
        y, z = shifted(x, 1, 0.0), shifted(a, 1, 1.0)
        y, z = y + z * end, z * open_end
        own.append((y, z))
        total += s1 + s2 * y
        squares += s3 + y * (2.0 * s4 + s5 * y)
        out[j, 0:1, :] = x[0:1] + a[0:1] * end[0:1]
        out[j, 1:2, :] = a[0:1]
        for k, part in enumerate((s2 * z, (s4 + s5 * y) * z, s5 * z * z)):
            out[j, 2 + k:3 + k, :] = jnp.sum(part, axis=0, keepdims=True)
        if j == last:
            out[j, 5:6, :] = jnp.sum(total, axis=0, keepdims=True)
            out[j, 6:7, :] = jnp.sum(squares, axis=0, keepdims=True)
        for g, (first, count) in enumerate(groups):
            if j == first + count - 1:
                if g == 0:
                    with scope("barw"):
                        far = jnp.where(is_root, num_tm * (num_env - 1), jnp.where(my_env == 0, 0, 1))
                        pl.semaphore_wait(barrier, num_tm - 1 + far)

                with scope(f"send{g}"):
                    @pl.when(jnp.logical_not(is_root))
                    def _(g=g):
                        root_copy(g).start()

                    for peer in peers:
                        link_copy(peer, g).start()

    with scope("linkw"):
        pending(link_sem.at[0], 2 * chunks * (num_tm - 1)).wait_recv()

    for j in range(chunks):
        y, z = own[j]
        carry = jnp.zeros((1, LANES), jnp.float32)
        mine = carry
        for t in range(num_tm - 1, 0, -1):
            carry = links[t, j, 0:1, :] + links[t, j, 1:2, :] * carry if t < num_tm - 1 else links[t, j, 0:1, :]
            mine = jnp.where(me == t - 1, carry, mine)
        c = y + z * jnp.where(top, 0.0, mine)

        def finish(i, state, j=j, c=c):
            for u in range(STEPS_UNROLLED):
                r = i * STEPS_UNROLLED + u
                rows = pl.ds(r, SEGMENTS, stride=pitch)
                adv = base[j, r] + prop[j, r] * c
                adv_ref[j, rows, :] = adv
                ret_ref[j, rows, :] = adv + val[j, r]
            return state

        with scope(f"fin{j}"):
            lax.fori_loop(0, seg_rows // STEPS_UNROLLED, finish, 0)

    def news_copy(t, e):
        return pltpu.make_async_remote_copy(
            src_ref=news.at[pl.ds(0, 2)], dst_ref=news.at[pl.ds(0, 2)],
            send_sem=news_sem.at[1], recv_sem=news_sem.at[0],
            device_id={"tm": t, "env": e}, device_id_type=MESH,
        )

    @pl.when(is_root)
    def _():
        for j in range(chunks):
            for r in range(ROWS if j == last else SUMS):
                table[root_tm, j, r, 0:1, :] = out[j, r:r + 1, :]
        sums = [jnp.zeros((num_env, LANES), jnp.float32)] * 2
        for g, (first, count) in enumerate(groups):
            with scope(f"rootw{g}"):
                pending(root_sem.at[g], sent_rows[g] * others, table).wait_recv()
            for j in range(first, first + count):
                carry = table[num_tm - 1, j, 0]
                for t in range(num_tm - 2, -1, -1):
                    sums[0] += table[t, j, 2] * carry
                    sums[1] += carry * (2.0 * table[t, j, 3] + table[t, j, 4] * carry)
                    if t:
                        carry = table[t, j, 0] + table[t, j, 1] * carry
        for t in range(num_tm):
            for k in range(2):
                sums[k] += table[t, last, SUMS + k]
        mean, square = (jnp.sum(s, keepdims=True) * (1.0 / cells) for s in sums)
        variance = square - mean * mean
        news[0:1, :] = jnp.broadcast_to(mean, (1, LANES))
        news[1:2, :] = jnp.broadcast_to(lax.rsqrt(variance + 1.0), (1, LANES))
        with scope("newsend"):
            for k in range(1, num_tm):
                news_copy((root_tm + num_tm - k) % num_tm, 0).start()

            def tell(e, state):
                for t in range(num_tm):
                    news_copy(t, e).start()
                return state

            lax.fori_loop(1, num_env, tell, 0)
        with scope("newsw"):
            pending(news_sem.at[1], 2 * others).wait_send()
            pending(send_sem.at[0], 2 * chunks * (num_tm - 1)).wait_send()

    @pl.when(jnp.logical_not(is_root))
    def _():
        with scope("sendw"):
            pending(send_sem.at[0], 2 * chunks * (num_tm - 1) + sum(sent_rows)).wait_send()
        with scope("newsr"):
            pending(news_sem.at[0], 2).wait_recv()

    stats_ref[0:2, :] = news[0:2, :]


def write_kernel(adv_ref, ret_ref, stats_ref, norm_hbm, ret_hbm, norm, sem):
    seg_rows = norm_hbm.shape[1]
    chunks = adv_ref.shape[0]
    pitch = seg_rows + PAD

    def out_copy(j, src, hbm, k):
        return pltpu.make_async_copy(
            src.at[j].reshape(SEGMENTS, pitch, LANES).at[:, pl.ds(0, seg_rows), :],
            hbm.at[:, :, pl.ds(j * LANES, LANES)],
            sem.at[k],
        )

    mean = jnp.broadcast_to(stats_ref[0:1, :], (8, LANES))
    scale = jnp.broadcast_to(stats_ref[1:2, :], (8, LANES))
    for j in range(chunks):
        out_copy(j, ret_ref, ret_hbm, 1).start()
    for j in range(chunks):
        for s in range(SEGMENTS):
            for r in range(0, seg_rows, 8):
                at = pl.ds(s * pitch + r, 8)
                norm[j, at, :] = (adv_ref[j, at, :] - mean) * scale
        out_copy(j, norm, norm_hbm, 0).start()
    pltpu.make_async_copy(ret_hbm, ret_hbm, sem.at[1]).wait()
    pltpu.make_async_copy(norm_hbm, norm_hbm, sem.at[0]).wait()


def local(num_tm, num_env, rewards, values, done_flags, bootstrap, discount_horizon, trace_horizon):
    steps, width = rewards.shape
    seg_rows, chunks = steps // SEGMENTS, width // LANES
    pitch = seg_rows + PAD
    split = lambda x: x.reshape(SEGMENTS, seg_rows, width)
    row = lambda x: x.reshape(1, width)
    padded = (chunks, SEGMENTS * pitch, LANES)
    tiles = (chunks, seg_rows, SEGMENTS, LANES)
    hbm = pl.BlockSpec(memory_space=pltpu.HBM)
    vmem = pl.BlockSpec(memory_space=pltpu.VMEM)
    f32 = jnp.float32
    handed = 4 * (2 * chunks * SEGMENTS * pitch + 8) * LANES
    adv, ret, stats = pl.pallas_call(
        functools.partial(exchange_kernel, num_tm, num_env, float(steps * width * num_tm * num_env)),
        out_shape=(pltpu.VMEM(padded, f32), pltpu.VMEM(padded, f32), pltpu.VMEM((8, LANES), f32)),
        in_specs=[hbm] * 6,
        out_specs=(vmem, vmem, vmem),
        scratch_shapes=[
            pltpu.VMEM(tiles, f32),
            pltpu.VMEM(tiles, f32),
            pltpu.VMEM(tiles, jnp.int32),
            pltpu.VMEM((3, 1, width), f32),
            pltpu.VMEM(tiles, f32),
            pltpu.VMEM(tiles, f32),
            pltpu.VMEM((chunks, 8, LANES), f32),
            pltpu.VMEM((num_tm, chunks, 8, LANES), f32),
            pltpu.VMEM((num_tm, chunks, ROWS, num_env, LANES), f32),
            pltpu.VMEM((8, LANES), f32),
            pltpu.SemaphoreType.DMA((1,)),
            pltpu.SemaphoreType.DMA((chunks,)),
            pltpu.SemaphoreType.DMA((1,)),
            pltpu.SemaphoreType.DMA((1,)),
            pltpu.SemaphoreType.DMA((len(send_groups(chunks)),)),
            pltpu.SemaphoreType.DMA((2,)),
        ],
        compiler_params=pltpu.CompilerParams(collective_id=0, has_side_effects=True, vmem_limit_bytes=VMEM_BYTES - handed),
    )(split(rewards), split(values), split(done_flags), row(bootstrap), row(discount_horizon), row(trace_horizon))
    norm_advantage, return_target = pl.pallas_call(
        write_kernel,
        out_shape=(jax.ShapeDtypeStruct((SEGMENTS, seg_rows, width), f32),) * 2,
        in_specs=[vmem] * 3,
        out_specs=(hbm, hbm),
        scratch_shapes=[pltpu.VMEM(padded, f32), pltpu.SemaphoreType.DMA((2,))],
        compiler_params=pltpu.CompilerParams(vmem_limit_bytes=8 * 2**20),
    )(*(pltpu.with_memory_space_constraint(x, pltpu.VMEM) for x in (adv, ret, stats)))
    return norm_advantage.reshape(steps, width), return_target.reshape(steps, width)


def solution(mesh):
    placed = (P("tm", "env"), P("tm", "env"), P("tm", "env"), P("env"), P("env"), P("env"))
    return jax.shard_map(
        functools.partial(local, mesh.shape["tm"], mesh.shape["env"]),
        mesh=mesh,
        in_specs=placed,
        out_specs=(P("tm", "env"), P("tm", "env")),
        check_vma=False,
    )
```

```python
import functools

import jax
import jax.numpy as jnp
from jax import lax
from jax.experimental import pallas as pl
from jax.experimental.pallas import tpu as pltpu
from jax.sharding import PartitionSpec as P

MESH = pl.DeviceIdType.MESH
SEGMENTS = 8
LANES = 128
PAD = 8
STEPS_UNROLLED = 32
VMEM_BYTES = 67043328
ROWS = 7
scope = jax.named_scope


def shifted(x, distance, fill):
    rows = lax.broadcasted_iota(jnp.int32, x.shape, 0)
    moved = pltpu.roll(x, SEGMENTS - distance, 0)
    return jnp.where(rows < SEGMENTS - distance, moved, fill)


def load_pieces(chunks):
    return [1] * (chunks - 1) + [2]


def send_groups(chunks):
    return ((0, chunks - 1), (chunks - 1, 1)) if chunks > 1 else ((0, 1),)


def exchange_kernel(
    num_tm, num_env, cells,
    rewards_hbm, values_hbm, flags_hbm, boot_hbm, disc_hbm, trace_hbm,
    adv_ref, ret_ref, stats_ref,
    rew, val, flg, params, base, prop, out, links, table, news,
    load_sem, link_sem, root_sem, news_sem,
):
    me = lax.axis_index("tm")
    my_env = lax.axis_index("env")
    seg_rows, width = rewards_hbm.shape[1], rewards_hbm.shape[2]
    chunks = width // LANES
    pitch = seg_rows + PAD
    groups = send_groups(chunks)
    last = chunks - 1
    pair = 2 if num_tm % 2 == 0 else 1
    others = num_tm * num_env - 1

    silent = [(t, 0) for t in range(pair)]
    middle = num_env // 2 - 1
    heralds = [(num_tm - 1, middle), (pair - 1, middle)]
    roots = silent + heralds
    told = [
        [(t, e) for e in range(num_env) for t in range(pair, num_tm)],
        [(t, e) for e in range(1, num_env) for t in range(pair)],
    ]

    def here(device):
        return jnp.logical_and(me == device[0], my_env == device[1])

    is_root = functools.reduce(jnp.logical_or, [here(r) for r in roots])
    serves = [me >= pair, me < pair]

    def at(device):
        return {"tm": device[0], "env": device[1]}

    def rows_of(ref, n):
        count = 1
        for d in ref.shape[:-1]:
            count *= d
        return ref.reshape(count, LANES).at[pl.ds(0, n)]

    def pending(sem, n, ref=base):
        part = rows_of(ref, n)
        return pltpu.make_async_remote_copy(
            src_ref=part, dst_ref=part, send_sem=sem, recv_sem=sem,
            device_id={"tm": lax.rem(me + 1, num_tm)}, device_id_type=MESH,
        )

    pieces = load_pieces(chunks)

    def load(j):
        size = seg_rows // pieces[j]
        for h in range(pieces[j]):
            rows = pl.ds((pieces[j] - 1 - h) * size, size)
            for s in range(SEGMENTS):
                for hbm, vmem in ((rewards_hbm, rew), (values_hbm, val), (flags_hbm, flg)):
                    pltpu.make_async_copy(
                        hbm.at[s, rows, pl.ds(j * LANES, LANES)], vmem.at[j, rows, s], load_sem.at[j + h]
                    ).start()

    load(0)
    barrier = pltpu.get_barrier_semaphore()
    for k in range(1, num_tm):
        pl.semaphore_signal(barrier, inc=1, device_id={"tm": lax.rem(me + k, num_tm)}, device_id_type=MESH)

    for herald, mine in zip(heralds, serves):
        @pl.when(functools.reduce(jnp.logical_and, [my_env != herald[1], mine, jnp.logical_not(is_root)]))
        def _(herald=herald):
            pl.semaphore_signal(barrier, inc=1, device_id=at(herald), device_id_type=MESH)

    for a, hbm in enumerate((boot_hbm, disc_hbm, trace_hbm)):
        pltpu.make_async_copy(hbm, params.at[a], load_sem.at[0]).start()
    for j in range(1, chunks):
        load(j)

    @pl.when(is_root)
    def _():
        def greet(k, state):
            for t in range(num_tm):
                pl.semaphore_signal(
                    barrier, inc=1, device_id=at((t, lax.rem(my_env + k, num_env))), device_id_type=MESH
                )
            return state

        lax.fori_loop(1, num_env, greet, 0)

    def link_copy(peer):
        return pltpu.make_async_remote_copy(
            src_ref=out.at[:, pl.ds(0, 2)], dst_ref=links.at[me, :, pl.ds(0, 2)],
            send_sem=load_sem.at[0], recv_sem=link_sem.at[0],
            device_id={"tm": peer}, device_id_type=MESH,
        )

    def sums_row(j):
        return 4 if j == chunks - 1 else 2

    def role_of(t):
        return 2 if t == num_tm - 1 else min(t, 1)

    def span(role, g):
        after = sums_row(groups[g][0] + groups[g][1] - 1)
        return ((2, after + 1), (0, after + 3), (1, after - 1))[role]

    def sent(role, g):
        return groups[g][1] * span(role, g)[1]

    roles = [me == 0, jnp.logical_and(me > 0, me < num_tm - 1), me == num_tm - 1]

    def root_copy(root, role, g):
        first, count = groups[g]
        rows = pl.ds(*span(role, g))
        return pltpu.make_async_remote_copy(
            src_ref=out.at[pl.ds(first, count), rows],
            dst_ref=table.at[me, pl.ds(first, count), rows, my_env],
            send_sem=load_sem.at[0], recv_sem=root_sem.at[g],
            device_id=at(root), device_id_type=MESH,
        )

    peers = [lax.rem(me + k, num_tm) for k in range(1, num_tm)]

    def send_block(devices, parts):
        for role in range(3):
            @pl.when(roles[role])
            def _(role=role):
                for root in devices:
                    if role_of(root[0]) != role:
                        for g in parts:
                            root_copy(root, role, g).start()
                    else:
                        @pl.when(jnp.logical_not(here(root)))
                        def _(root=root):
                            for g in parts:
                                root_copy(root, role, g).start()

    with scope("ldw00"):
        pending(load_sem.at[0], 3 * chunks + 3 * (seg_rows // pieces[0]) * SEGMENTS).wait_recv()
    inv_trace = 1.0 / (1.0 - 1.0 / params[2])
    discount = 1.0 - 1.0 / params[1]
    rate_all = discount * (1.0 - 1.0 / params[2])
    top = me == num_tm - 1
    ends = jnp.where(top, params[0] * inv_trace, 0.0)
    open_end = jnp.where(top, 0.0, 1.0)

    own = []
    zero = jnp.zeros((SEGMENTS, LANES), jnp.float32)
    total, squares = zero, zero
    for j in range(chunks):
        spread = lambda x: jnp.broadcast_to(x[:, j * LANES:(j + 1) * LANES], zero.shape)
        disc, rate, itr, end = spread(discount), spread(rate_all), spread(inv_trace), spread(ends)

        def steps(i, state, last_row, j=j, disc=disc, rate=rate):
            b, p, nv, s1, s2, s3, s4, s5 = state
            for u in range(STEPS_UNROLLED):
                r = last_row - (i * STEPS_UNROLLED + u)
                v = val[j, r]
                live = flg[j, r] == 0
                d = jnp.where(live, disc, 0.0)
                g = jnp.where(live, rate, 0.0)
                b = (rew[j, r] - v + d * nv) + g * b
                p = g * p
                nv = v
                base[j, r] = b
                prop[j, r] = p
                s1, s2, s3, s4, s5 = s1 + b, s2 + p, s3 + b * b, s4 + b * p, s5 + p * p
            return b, p, nv, s1, s2, s3, s4, s5

        state = (zero, zero + 1.0, zero) + (zero,) * 5
        size = seg_rows // pieces[j]
        for h in range(pieces[j]):
            if j + h:
                with scope(f"ldw{j}{h}"):
                    pending(load_sem.at[j + h], 3 * size * SEGMENTS).wait_recv()
            with scope(f"scan{j}{h}"):
                scan = functools.partial(steps, last_row=seg_rows - 1 - h * size)
                state = lax.fori_loop(0, size // STEPS_UNROLLED, scan, state)
        b, p, v, s1, s2, s3, s4, s5 = state
        x, a = b + v * itr, p
        for d in (1, 2, 4):
            x_next, a_next = shifted(x, d, 0.0), shifted(a, d, 1.0)
            x, a = x + a * x_next, a * a_next
        y, z = shifted(x, 1, 0.0), shifted(a, 1, 1.0)
        y, z = y + z * end, z * open_end
        own.append((y, z))
        total += s1 + s2 * y
        squares += s3 + y * (2.0 * s4 + s5 * y)
        out[j, 0:1, :] = a[0:1]
        out[j, 1:2, :] = x[0:1] + a[0:1] * end[0:1]
        for k, part in enumerate((s2 * z, (s4 + s5 * y) * z, s5 * z * z)):
            out[j, sums_row(j) + k:sums_row(j) + k + 1, :] = jnp.sum(part, axis=0, keepdims=True)
        if j == last:
            out[j, 2:3, :] = jnp.sum(total, axis=0, keepdims=True)
            out[j, 3:4, :] = jnp.sum(squares, axis=0, keepdims=True)
        for g, (first, count) in enumerate(groups):
            if j == first + count - 1:
                if g == 0:
                    with scope("barw"):
                        far = sum(jnp.where(my_env == env, 0, 1) for _, env in roots)
                        for herald, devices in zip(heralds, told):
                            answers = sum(d[1] != herald[1] and d not in roots for d in devices)
                            far += jnp.where(here(herald), answers, 0)
                        pl.semaphore_wait(barrier, num_tm - 1 + far)

                with scope(f"send{g}"):
                    send_block(silent, [g])

    with scope("send2"):
        send_block(heralds, range(len(groups)))
        for peer in peers:
            link_copy(peer).start()

    with scope("linkw"):
        pending(link_sem.at[0], 2 * chunks * (num_tm - 1)).wait_recv()

    for j in range(chunks):
        y, z = own[j]
        carry = jnp.zeros((1, LANES), jnp.float32)
        mine = carry
        for t in range(num_tm - 1, 0, -1):
            carry = links[t, j, 1:2, :] + links[t, j, 0:1, :] * carry if t < num_tm - 1 else links[t, j, 1:2, :]
            mine = jnp.where(me == t - 1, carry, mine)
        c = y + z * jnp.where(top, 0.0, mine)

        def finish(i, state, j=j, c=c):
            for u in range(STEPS_UNROLLED):
                r = i * STEPS_UNROLLED + u
                rows = pl.ds(r, SEGMENTS, stride=pitch)
                adv = base[j, r] + prop[j, r] * c
                adv_ref[j, rows, :] = adv
                ret_ref[j, rows, :] = adv + val[j, r]
            return state

        with scope(f"fin{j}"):
            lax.fori_loop(0, seg_rows // STEPS_UNROLLED, finish, 0)

    def news_copy(t, e):
        return pltpu.make_async_remote_copy(
            src_ref=news.at[pl.ds(0, 2)], dst_ref=news.at[pl.ds(0, 2)],
            send_sem=load_sem.at[1], recv_sem=news_sem.at[0],
            device_id=at((t, e)), device_id_type=MESH,
        )

    link_rows = 2 * chunks * (num_tm - 1)

    @pl.when(is_root)
    def _():
        for j in range(chunks):
            for r in range(sums_row(j) + 3):
                table[me, j, r, pl.ds(my_env, 1), :] = out[j, r:r + 1, :]
        sums = [jnp.zeros((num_env, LANES), jnp.float32)] * 2
        for g, (first, count) in enumerate(groups):
            with scope(f"rootw{g}"):
                everyone = num_env * sum(sent(role_of(t), g) for t in range(num_tm))
                for role in sorted({role_of(root[0]) for root in roots}):
                    @pl.when(roles[role])
                    def _(role=role):
                        pending(root_sem.at[g], everyone - sent(role, g), table).wait_recv()
            for j in range(first, first + count):
                first_sum = sums_row(j)
                carry = table[num_tm - 1, j, 1]
                for t in range(num_tm - 2, -1, -1):
                    sums[0] += table[t, j, first_sum] * carry
                    sums[1] += carry * (2.0 * table[t, j, first_sum + 1] + table[t, j, first_sum + 2] * carry)
                    if t:
                        carry = table[t, j, 1] + table[t, j, 0] * carry
        for t in range(num_tm):
            for k in range(2):
                sums[k] += table[t, last, 2 + k]
        mean, square = (jnp.sum(s, keepdims=True) * (1.0 / cells) for s in sums)
        variance = square - mean * mean
        news[0:1, :] = jnp.broadcast_to(mean, (1, LANES))
        news[1:2, :] = jnp.broadcast_to(lax.rsqrt(variance + 1.0), (1, LANES))

    for herald, devices in zip(heralds, told):
        @pl.when(here(herald))
        def _(herald=herald, devices=devices):
            listeners = [d for d in devices if d not in roots]
            with scope("newsend"):
                for t, e in listeners:
                    news_copy(t, e).start()
            with scope("newsw"):
                pending(load_sem.at[1], 2 * len(listeners)).wait_send()

    with scope("sendw"):
        for role in range(3):
            block = sum(sent(role, g) for g in range(len(groups)))

            @pl.when(jnp.logical_and(roles[role], is_root))
            def _(block=block):
                pending(load_sem.at[0], link_rows + (len(roots) - 1) * block).wait_send()

            @pl.when(jnp.logical_and(roles[role], jnp.logical_not(is_root)))
            def _(block=block):
                pending(load_sem.at[0], link_rows + len(roots) * block).wait_send()

    @pl.when(jnp.logical_not(is_root))
    def _():
        with scope("newsr"):
            pending(news_sem.at[0], 2).wait_recv()

    stats_ref[0:2, :] = news[0:2, :]


def write_kernel(adv_ref, ret_ref, stats_ref, norm_hbm, ret_hbm, norm, sem):
    seg_rows = norm_hbm.shape[1]
    chunks = adv_ref.shape[0]
    pitch = seg_rows + PAD

    def out_copy(j, src, hbm, k):
        return pltpu.make_async_copy(
            src.at[j].reshape(SEGMENTS, pitch, LANES).at[:, pl.ds(0, seg_rows), :],
            hbm.at[:, :, pl.ds(j * LANES, LANES)],
            sem.at[k],
        )

    mean = jnp.broadcast_to(stats_ref[0:1, :], (8, LANES))
    scale = jnp.broadcast_to(stats_ref[1:2, :], (8, LANES))
    for j in range(chunks):
        out_copy(j, ret_ref, ret_hbm, 1).start()
    for j in range(chunks):
        for s in range(SEGMENTS):
            for r in range(0, seg_rows, 8):
                at = pl.ds(s * pitch + r, 8)
                norm[j, at, :] = (adv_ref[j, at, :] - mean) * scale
        out_copy(j, norm, norm_hbm, 0).start()
    pltpu.make_async_copy(ret_hbm, ret_hbm, sem.at[1]).wait()
    pltpu.make_async_copy(norm_hbm, norm_hbm, sem.at[0]).wait()


def local(num_tm, num_env, rewards, values, done_flags, bootstrap, discount_horizon, trace_horizon):
    steps, width = rewards.shape
    seg_rows, chunks = steps // SEGMENTS, width // LANES
    pitch = seg_rows + PAD
    split = lambda x: x.reshape(SEGMENTS, seg_rows, width)
    row = lambda x: x.reshape(1, width)
    padded = (chunks, SEGMENTS * pitch, LANES)
    tiles = (chunks, seg_rows, SEGMENTS, LANES)
    hbm = pl.BlockSpec(memory_space=pltpu.HBM)
    vmem = pl.BlockSpec(memory_space=pltpu.VMEM)
    f32 = jnp.float32
    handed = 4 * (2 * chunks * SEGMENTS * pitch + 8) * LANES
    adv, ret, stats = pl.pallas_call(
        functools.partial(exchange_kernel, num_tm, num_env, float(steps * width * num_tm * num_env)),
        out_shape=(pltpu.VMEM(padded, f32), pltpu.VMEM(padded, f32), pltpu.VMEM((8, LANES), f32)),
        in_specs=[hbm] * 6,
        out_specs=(vmem, vmem, vmem),
        scratch_shapes=[
            pltpu.VMEM(tiles, f32),
            pltpu.VMEM(tiles, f32),
            pltpu.VMEM(tiles, jnp.int32),
            pltpu.VMEM((3, 1, width), f32),
            pltpu.VMEM(tiles, f32),
            pltpu.VMEM(tiles, f32),
            pltpu.VMEM((chunks, 8, LANES), f32),
            pltpu.VMEM((num_tm, chunks, 8, LANES), f32),
            pltpu.VMEM((num_tm, chunks, ROWS, num_env, LANES), f32),
            pltpu.VMEM((8, LANES), f32),
            pltpu.SemaphoreType.DMA((sum(load_pieces(chunks)),)),
            pltpu.SemaphoreType.DMA((1,)),
            pltpu.SemaphoreType.DMA((len(send_groups(chunks)),)),
            pltpu.SemaphoreType.DMA((1,)),
        ],
        compiler_params=pltpu.CompilerParams(collective_id=0, has_side_effects=True, vmem_limit_bytes=VMEM_BYTES - handed),
    )(split(rewards), split(values), split(done_flags), row(bootstrap), row(discount_horizon), row(trace_horizon))
    norm_advantage, return_target = pl.pallas_call(
        write_kernel,
        out_shape=(jax.ShapeDtypeStruct((SEGMENTS, seg_rows, width), f32),) * 2,
        in_specs=[vmem] * 3,
        out_specs=(hbm, hbm),
        scratch_shapes=[pltpu.VMEM(padded, f32), pltpu.SemaphoreType.DMA((2,))],
        compiler_params=pltpu.CompilerParams(vmem_limit_bytes=8 * 2**20),
    )(*(pltpu.with_memory_space_constraint(x, pltpu.VMEM) for x in (adv, ret, stats)))
    return norm_advantage.reshape(steps, width), return_target.reshape(steps, width)


def solution(mesh):
    placed = (P("tm", "env"), P("tm", "env"), P("tm", "env"), P("env"), P("env"), P("env"))
    return jax.shard_map(
        functools.partial(local, mesh.shape["tm"], mesh.shape["env"]),
        mesh=mesh,
        in_specs=placed,
        out_specs=(P("tm", "env"), P("tm", "env")),
        check_vma=False,
    )
```

```python
import functools

import jax
import jax.numpy as jnp
from jax import lax
from jax.experimental import pallas as pl
from jax.experimental.pallas import tpu as pltpu
from jax.sharding import PartitionSpec as P

MESH = pl.DeviceIdType.MESH
SEGMENTS = 8
LANES = 128
PAD = 8
STEPS_UNROLLED = 32
VMEM_BYTES = 67043328
ROWS = 7
scope = jax.named_scope


def shifted(x, distance, fill):
    rows = lax.broadcasted_iota(jnp.int32, x.shape, 0)
    moved = pltpu.roll(x, SEGMENTS - distance, 0)
    return jnp.where(rows < SEGMENTS - distance, moved, fill)


def load_pieces(chunks):
    return [1] * (chunks - 1) + [2]


def send_groups(chunks):
    return ((0, chunks - 1), (chunks - 1, 1)) if chunks > 1 else ((0, 1),)


def exchange_kernel(
    num_tm, num_env,
    rewards_hbm, values_hbm, flags_hbm, boot_hbm, disc_hbm, trace_hbm,
    adv_ref, ret_ref, stats_ref,
    rew, val, flg, params, base, prop, out, links, table, news,
    link_sem, root_sem, news_sem,
):
    me = lax.axis_index("tm")
    my_env = lax.axis_index("env")
    seg_rows, width = rewards_hbm.shape[1], rewards_hbm.shape[2]
    chunks = width // LANES
    pitch = seg_rows + PAD
    groups = send_groups(chunks)
    last = chunks - 1
    pair = 2 if num_tm % 2 == 0 else 1
    others = num_tm * num_env - 1

    silent = [(t, 0) for t in range(pair)]
    middle = num_env // 2 - 1
    heralds = [(num_tm - 1, middle), (pair - 1, middle)]
    roots = silent + heralds
    told = [
        [(t, e) for e in range(num_env) for t in range(pair, num_tm)],
        [(t, e) for e in range(1, num_env) for t in range(pair)],
    ]

    def here(device):
        return jnp.logical_and(me == device[0], my_env == device[1])

    is_root = functools.reduce(jnp.logical_or, [here(r) for r in roots])
    serves = [me >= pair, me < pair]

    def at(device):
        return {"tm": device[0], "env": device[1]}

    def rows_of(ref, n):
        count = 1
        for d in ref.shape[:-1]:
            count *= d
        return ref.reshape(count, LANES).at[pl.ds(0, n)]

    def pending(sem, n, ref=base):
        part = rows_of(ref, n)
        return pltpu.make_async_remote_copy(
            src_ref=part, dst_ref=part, send_sem=sem, recv_sem=sem,
            device_id={"tm": lax.rem(me + 1, num_tm)}, device_id_type=MESH,
        )

    def sums_row(j):
        return 4 if j == chunks - 1 else 2

    def role_of(t):
        return 2 if t == num_tm - 1 else min(t, 1)

    def span(role, g):
        after = sums_row(groups[g][0] + groups[g][1] - 1)
        return ((2, after + 1), (0, after + 3), (1, after - 1))[role]

    def sent(role, g):
        return groups[g][1] * span(role, g)[1]

    roles = [me == 0, jnp.logical_and(me > 0, me < num_tm - 1), me == num_tm - 1]

    link_rows = 2 * chunks * (num_tm - 1)

    def scan_and_send(load_sem):
        pieces = load_pieces(chunks)
        at_piece = [sum(pieces[:j]) for j in range(chunks)]

        def load(j):
            size = seg_rows // pieces[j]
            for h in range(pieces[j]):
                rows = pl.ds((pieces[j] - 1 - h) * size, size)
                for s in range(SEGMENTS):
                    for hbm, vmem in ((rewards_hbm, rew), (values_hbm, val), (flags_hbm, flg)):
                        pltpu.make_async_copy(
                            hbm.at[s, rows, pl.ds(j * LANES, LANES)], vmem.at[j, rows, s], load_sem.at[at_piece[j] + h]
                        ).start()

        load(0)
        barrier = pltpu.get_barrier_semaphore()
        for k in range(1, num_tm):
            pl.semaphore_signal(barrier, inc=1, device_id={"tm": lax.rem(me + k, num_tm)}, device_id_type=MESH)

        for herald, mine in zip(heralds, serves):
            @pl.when(functools.reduce(jnp.logical_and, [my_env != herald[1], mine, jnp.logical_not(is_root)]))
            def _(herald=herald):
                pl.semaphore_signal(barrier, inc=1, device_id=at(herald), device_id_type=MESH)

        for a, hbm in enumerate((boot_hbm, disc_hbm, trace_hbm)):
            pltpu.make_async_copy(hbm, params.at[a], load_sem.at[0]).start()
        for j in range(1, chunks):
            load(j)

        @pl.when(is_root)
        def _():
            def greet(k, state):
                for t in range(num_tm):
                    pl.semaphore_signal(
                        barrier, inc=1, device_id=at((t, lax.rem(my_env + k, num_env))), device_id_type=MESH
                    )
                return state

            lax.fori_loop(1, num_env, greet, 0)

        def link_copy(peer):
            return pltpu.make_async_remote_copy(
                src_ref=out.at[:, pl.ds(0, 2)], dst_ref=links.at[me, :, pl.ds(0, 2)],
                send_sem=load_sem.at[0], recv_sem=link_sem.at[0],
                device_id={"tm": peer}, device_id_type=MESH,
            )

        def root_copy(root, role, g):
            first, count = groups[g]
            rows = pl.ds(*span(role, g))
            return pltpu.make_async_remote_copy(
                src_ref=out.at[pl.ds(first, count), rows],
                dst_ref=table.at[me, pl.ds(first, count), rows, my_env],
                send_sem=load_sem.at[0], recv_sem=root_sem.at[g],
                device_id=at(root), device_id_type=MESH,
            )

        peers = [lax.rem(me + k, num_tm) for k in range(1, num_tm)]

        def send_block(devices, parts):
            for role in range(3):
                @pl.when(roles[role])
                def _(role=role):
                    for root in devices:
                        if role_of(root[0]) != role:
                            for g in parts:
                                root_copy(root, role, g).start()
                        else:
                            @pl.when(jnp.logical_not(here(root)))
                            def _(root=root):
                                for g in parts:
                                    root_copy(root, role, g).start()

        with scope("ldw00"):
            pending(load_sem.at[0], 3 * chunks + 3 * (seg_rows // pieces[0]) * SEGMENTS).wait_recv()
        inv_trace = 1.0 / (1.0 - 1.0 / params[2])
        discount = 1.0 - 1.0 / params[1]
        rate_all = discount * (1.0 - 1.0 / params[2])
        top = me == num_tm - 1
        ends = jnp.where(top, params[0] * inv_trace, 0.0)
        open_end = jnp.where(top, 0.0, 1.0)

        own = []
        zero = jnp.zeros((SEGMENTS, LANES), jnp.float32)
        total, squares = zero, zero
        for j in range(chunks):
            spread = lambda x: jnp.broadcast_to(x[:, j * LANES:(j + 1) * LANES], zero.shape)
            disc, rate, itr, end = spread(discount), spread(rate_all), spread(inv_trace), spread(ends)

            def steps(i, state, last_row, j=j, disc=disc, rate=rate):
                b, p, nv, s1, s2, s3, s4, s5 = state
                for u in range(STEPS_UNROLLED):
                    r = last_row - (i * STEPS_UNROLLED + u)
                    v = val[j, r]
                    live = flg[j, r] == 0
                    d = jnp.where(live, disc, 0.0)
                    g = jnp.where(live, rate, 0.0)
                    b = (rew[j, r] - v + d * nv) + g * b
                    p = g * p
                    nv = v
                    base[j, r] = b
                    prop[j, r] = p
                    s1, s2, s3, s4, s5 = s1 + b, s2 + p, s3 + b * b, s4 + b * p, s5 + p * p
                return b, p, nv, s1, s2, s3, s4, s5

            state = (zero, zero + 1.0, zero) + (zero,) * 5
            size = seg_rows // pieces[j]
            for h in range(pieces[j]):
                if j == last and h == pieces[j] - 1:
                    with scope("barw"):
                        far = sum(jnp.where(my_env == env, 0, 1) for _, env in roots)
                        for herald, devices in zip(heralds, told):
                            answers = sum(d[1] != herald[1] and d not in roots for d in devices)
                            far += jnp.where(here(herald), answers, 0)
                        pl.semaphore_wait(barrier, num_tm - 1 + far)
                    if chunks > 1:
                        with scope("send0"):
                            send_block(silent, [0])
                if j + h:
                    with scope(f"ldw{j}{h}"):
                        pending(load_sem.at[at_piece[j] + h], 3 * size * SEGMENTS).wait_recv()
                with scope(f"scan{j}{h}"):
                    scan = functools.partial(steps, last_row=seg_rows - 1 - h * size)
                    state = lax.fori_loop(0, size // STEPS_UNROLLED, scan, state)
            b, p, v, s1, s2, s3, s4, s5 = state
            x, a = b + v * itr, p
            for d in (1, 2, 4):
                x_next, a_next = shifted(x, d, 0.0), shifted(a, d, 1.0)
                x, a = x + a * x_next, a * a_next
            y, z = shifted(x, 1, 0.0), shifted(a, 1, 1.0)
            y, z = y + z * end, z * open_end
            own.append((y, z))
            total += s1 + s2 * y
            squares += s3 + y * (2.0 * s4 + s5 * y)
            out[j, 0:1, :] = a[0:1]
            out[j, 1:2, :] = x[0:1] + a[0:1] * end[0:1]
            for k, part in enumerate((s2 * z, (s4 + s5 * y) * z, s5 * z * z)):
                out[j, sums_row(j) + k:sums_row(j) + k + 1, :] = jnp.sum(part, axis=0, keepdims=True)
            if j == last:
                out[j, 2:3, :] = jnp.sum(total, axis=0, keepdims=True)
                out[j, 3:4, :] = jnp.sum(squares, axis=0, keepdims=True)
        with scope("send1"):
            send_block(silent, [len(groups) - 1])
        with scope("send2"):
            send_block(heralds, range(len(groups)))
            for peer in peers:
                link_copy(peer).start()

        with scope("linkw"):
            pending(link_sem.at[0], 2 * chunks * (num_tm - 1)).wait_recv()

        for j in range(chunks):
            y, z = own[j]
            carry = jnp.zeros((1, LANES), jnp.float32)
            mine = carry
            for t in range(num_tm - 1, 0, -1):
                carry = links[t, j, 1:2, :] + links[t, j, 0:1, :] * carry if t < num_tm - 1 else links[t, j, 1:2, :]
                mine = jnp.where(me == t - 1, carry, mine)
            c = y + z * jnp.where(top, 0.0, mine)

            def finish(i, state, j=j, c=c):
                for u in range(STEPS_UNROLLED):
                    r = i * STEPS_UNROLLED + u
                    rows = pl.ds(r, SEGMENTS, stride=pitch)
                    adv = base[j, r] + prop[j, r] * c
                    adv_ref[j, rows, :] = adv
                    ret_ref[j, rows, :] = adv + val[j, r]
                return state

            with scope(f"fin{j}"):
                lax.fori_loop(0, seg_rows // STEPS_UNROLLED, finish, 0)

        with scope("sendw"):
            for role in range(3):
                block = sum(sent(role, g) for g in range(len(groups)))

                @pl.when(jnp.logical_and(roles[role], is_root))
                def _(block=block):
                    pending(load_sem.at[0], link_rows + (len(roots) - 1) * block).wait_send()

                @pl.when(jnp.logical_and(roles[role], jnp.logical_not(is_root)))
                def _(block=block):
                    pending(load_sem.at[0], link_rows + len(roots) * block).wait_send()

    pl.run_scoped(scan_and_send, pltpu.SemaphoreType.DMA((sum(load_pieces(chunks)),)))

    def news_copy(t, e):
        return pltpu.make_async_remote_copy(
            src_ref=news.at[pl.ds(0, 2)], dst_ref=news.at[pl.ds(0, 2)],
            send_sem=link_sem.at[0], recv_sem=news_sem.at[0],
            device_id=at((t, e)), device_id_type=MESH,
        )

    @pl.when(is_root)
    def _():
        for j in range(chunks):
            for r in range(sums_row(j) + 3):
                table[me, j, r, pl.ds(my_env, 1), :] = out[j, r:r + 1, :]
        sums = [jnp.zeros((num_env, LANES), jnp.float32)] * 2
        for g, (first, count) in enumerate(groups):
            with scope(f"rootw{g}"):
                everyone = num_env * sum(sent(role_of(t), g) for t in range(num_tm))
                for role in sorted({role_of(root[0]) for root in roots}):
                    @pl.when(roles[role])
                    def _(role=role):
                        pending(root_sem.at[g], everyone - sent(role, g), table).wait_recv()
            for j in range(first, first + count):
                first_sum = sums_row(j)
                carry = table[num_tm - 1, j, 1]
                for t in range(num_tm - 2, -1, -1):
                    sums[0] += table[t, j, first_sum] * carry
                    sums[1] += carry * (2.0 * table[t, j, first_sum + 1] + table[t, j, first_sum + 2] * carry)
                    if t:
                        carry = table[t, j, 1] + table[t, j, 0] * carry
        for t in range(num_tm):
            for k in range(2):
                sums[k] += table[t, last, 2 + k]
        for k in range(2):
            news[k:k + 1, :] = jnp.sum(sums[k], axis=0, keepdims=True)

    for herald, devices in zip(heralds, told):
        @pl.when(here(herald))
        def _(herald=herald, devices=devices):
            listeners = [d for d in devices if d not in roots]
            with scope("newsend"):
                for t, e in listeners:
                    if e == 0 or e == herald[1]:
                        news_copy(t, e).start()

                def tell(k, state):
                    e = jnp.where(k < herald[1], k, k + 1)
                    for t in sorted({t for t, _ in devices}):
                        news_copy(t, e).start()
                    return state

                lax.fori_loop(1, num_env - 1, tell, 0)
            with scope("newsw"):
                pending(link_sem.at[0], 2 * len(listeners)).wait_send()

    @pl.when(jnp.logical_not(is_root))
    def _():
        with scope("newsr"):
            pending(news_sem.at[0], 2).wait_recv()

    stats_ref[0:2, :] = news[0:2, :]


def write_kernel(cells, *refs):
    pl.run_scoped(functools.partial(write, cells, *refs), pltpu.SemaphoreType.DMA((2,)))


def write(cells, adv_ref, ret_ref, stats_ref, norm_hbm, ret_hbm, norm, sem):
    seg_rows = norm_hbm.shape[1]
    chunks = adv_ref.shape[0]
    pitch = seg_rows + PAD

    def out_copy(j, src, hbm, k):
        return pltpu.make_async_copy(
            src.at[j].reshape(SEGMENTS, pitch, LANES).at[:, pl.ds(0, seg_rows), :],
            hbm.at[:, :, pl.ds(j * LANES, LANES)],
            sem.at[k],
        )

    for j in range(chunks):
        out_copy(j, ret_ref, ret_hbm, 1).start()
    moments = jnp.sum(stats_ref[0:2, :], axis=1, keepdims=True) * (1.0 / cells)
    mean = moments[0:1]
    scale = lax.rsqrt(moments[1:2] - mean * mean + 1.0)
    mean = jnp.broadcast_to(mean, (8, LANES))
    scale = jnp.broadcast_to(scale, (8, LANES))
    for j in range(chunks):
        for s in range(SEGMENTS):
            for r in range(0, seg_rows, 8):
                at = pl.ds(s * pitch + r, 8)
                norm[j, at, :] = (adv_ref[j, at, :] - mean) * scale
        out_copy(j, norm, norm_hbm, 0).start()
    pltpu.make_async_copy(ret_hbm, ret_hbm, sem.at[1]).wait()
    pltpu.make_async_copy(norm_hbm, norm_hbm, sem.at[0]).wait()


def local(num_tm, num_env, rewards, values, done_flags, bootstrap, discount_horizon, trace_horizon):
    steps, width = rewards.shape
    seg_rows, chunks = steps // SEGMENTS, width // LANES
    pitch = seg_rows + PAD
    split = lambda x: x.reshape(SEGMENTS, seg_rows, width)
    row = lambda x: x.reshape(1, width)
    padded = (chunks, SEGMENTS * pitch, LANES)
    tiles = (chunks, seg_rows, SEGMENTS, LANES)
    hbm = pl.BlockSpec(memory_space=pltpu.HBM)
    vmem = pl.BlockSpec(memory_space=pltpu.VMEM)
    f32 = jnp.float32
    handed = 4 * (2 * chunks * SEGMENTS * pitch + 8) * LANES
    adv, ret, stats = pl.pallas_call(
        functools.partial(exchange_kernel, num_tm, num_env),
        out_shape=(pltpu.VMEM(padded, f32), pltpu.VMEM(padded, f32), pltpu.VMEM((8, LANES), f32)),
        in_specs=[hbm] * 6,
        out_specs=(vmem, vmem, vmem),
        scratch_shapes=[
            pltpu.VMEM(tiles, f32),
            pltpu.VMEM(tiles, f32),
            pltpu.VMEM(tiles, jnp.int32),
            pltpu.VMEM((3, 1, width), f32),
            pltpu.VMEM(tiles, f32),
            pltpu.VMEM(tiles, f32),
            pltpu.VMEM((chunks, 8, LANES), f32),
            pltpu.VMEM((num_tm, chunks, 8, LANES), f32),
            pltpu.VMEM((num_tm, chunks, ROWS, num_env, LANES), f32),
            pltpu.VMEM((8, LANES), f32),
            pltpu.SemaphoreType.DMA((1,)),
            pltpu.SemaphoreType.DMA((len(send_groups(chunks)),)),
            pltpu.SemaphoreType.DMA((1,)),
        ],
        compiler_params=pltpu.CompilerParams(collective_id=0, has_side_effects=True, vmem_limit_bytes=VMEM_BYTES - handed),
    )(split(rewards), split(values), split(done_flags), row(bootstrap), row(discount_horizon), row(trace_horizon))
    norm_advantage, return_target = pl.pallas_call(
        functools.partial(write_kernel, float(steps * width * num_tm * num_env)),
        out_shape=(jax.ShapeDtypeStruct((SEGMENTS, seg_rows, width), f32),) * 2,
        in_specs=[vmem] * 3,
        out_specs=(hbm, hbm),
        scratch_shapes=[pltpu.VMEM(padded, f32)],
        compiler_params=pltpu.CompilerParams(vmem_limit_bytes=8 * 2**20),
    )(*(pltpu.with_memory_space_constraint(x, pltpu.VMEM) for x in (adv, ret, stats)))
    return norm_advantage.reshape(steps, width), return_target.reshape(steps, width)


def solution(mesh):
    placed = (P("tm", "env"), P("tm", "env"), P("tm", "env"), P("env"), P("env"), P("env"))
    return jax.shard_map(
        functools.partial(local, mesh.shape["tm"], mesh.shape["env"]),
        mesh=mesh,
        in_specs=placed,
        out_specs=(P("tm", "env"), P("tm", "env")),
        check_vma=False,
    )
```

```python
import functools

import jax
import jax.numpy as jnp
from jax import lax
from jax.experimental import pallas as pl
from jax.experimental.pallas import tpu as pltpu
from jax.sharding import PartitionSpec as P

MESH = pl.DeviceIdType.MESH
SEGMENTS = 8
LANES = 128
PAD = 8
STEPS_UNROLLED = 64
VMEM_BYTES = 67043328
ROWS = 7
scope = jax.named_scope


def shifted(x, distance, fill):
    rows = lax.broadcasted_iota(jnp.int32, x.shape, 0)
    moved = pltpu.roll(x, SEGMENTS - distance, 0)
    return jnp.where(rows < SEGMENTS - distance, moved, fill)


def load_pieces(chunks):
    return [1] * (chunks - 1) + [2]


def send_groups(chunks):
    cuts = sorted({0, max(chunks - 2, 0), chunks - 1})
    return tuple((a, b - a) for a, b in zip(cuts, cuts[1:] + [chunks]))


def exchange_kernel(
    num_tm, num_env,
    rewards_hbm, values_hbm, flags_hbm, boot_hbm, disc_hbm, trace_hbm,
    adv_ref, ret_ref, stats_ref,
    rew, val, flg, params, base, prop, out, links, table, news,
    link_sem, root_sem,
):
    me = lax.axis_index("tm")
    my_env = lax.axis_index("env")
    seg_rows, width = rewards_hbm.shape[1], rewards_hbm.shape[2]
    chunks = width // LANES
    pitch = seg_rows + PAD
    groups = send_groups(chunks)
    last = chunks - 1
    pair = 2 if num_tm % 2 == 0 else 1
    others = num_tm * num_env - 1

    silent = [(t, 0) for t in range(pair)]
    middle = num_env // 2 - 1
    heralds = [(num_tm - 1, middle), (pair - 1, middle)]
    if num_tm == pair:
        heralds = heralds[1:]
    roots = silent + heralds
    told = [
        [(t, e) for e in range(num_env) for t in range(pair, num_tm)],
        [(t, e) for e in range(1, num_env) for t in range(pair)],
    ][-len(heralds):]

    def here(device):
        return jnp.logical_and(me == device[0], my_env == device[1])

    is_root = functools.reduce(jnp.logical_or, [here(r) for r in roots])
    serves = [me >= pair, me < pair][-len(heralds):]

    def at(device):
        return {"tm": device[0], "env": device[1]}

    def rows_of(ref, n):
        count = 1
        for d in ref.shape[:-1]:
            count *= d
        return ref.reshape(count, LANES).at[pl.ds(0, n)]

    def pending(sem, n, ref=base):
        part = rows_of(ref, n)
        return pltpu.make_async_remote_copy(
            src_ref=part, dst_ref=part, send_sem=sem, recv_sem=sem,
            device_id={"tm": lax.rem(me + 1, num_tm)}, device_id_type=MESH,
        )

    def sums_row(j):
        return 4 if j == chunks - 1 else 2

    def role_of(t):
        return 2 if t == num_tm - 1 else min(t, 1)

    def span(role, g):
        after = sums_row(groups[g][0] + groups[g][1] - 1)
        return ((2, after + 1), (0, after + 3), (1, after - 1))[role]

    def sent(role, g):
        return groups[g][1] * span(role, g)[1]

    roles = [me == 0, jnp.logical_and(me > 0, me < num_tm - 1), me == num_tm - 1]

    link_rows = 2 * chunks * (num_tm - 1)

    def scan_and_send(load_sem):
        pieces = load_pieces(chunks)
        at_piece = [sum(pieces[:j]) for j in range(chunks)]

        def load(j):
            size = seg_rows // pieces[j]
            for h in range(pieces[j]):
                rows = pl.ds((pieces[j] - 1 - h) * size, size)
                for s in range(SEGMENTS):
                    for hbm, vmem in ((rewards_hbm, rew), (values_hbm, val), (flags_hbm, flg)):
                        pltpu.make_async_copy(
                            hbm.at[s, rows, pl.ds(j * LANES, LANES)], vmem.at[j, rows, s], load_sem.at[at_piece[j] + h]
                        ).start()

        load(0)
        for a, hbm in enumerate((boot_hbm, disc_hbm, trace_hbm)):
            pltpu.make_async_copy(hbm, params.at[a], load_sem.at[0]).start()
        for j in range(1, chunks):
            load(j)
        barrier = pltpu.get_barrier_semaphore()
        for k in range(1, num_tm):
            pl.semaphore_signal(barrier, inc=1, device_id={"tm": lax.rem(me + k, num_tm)}, device_id_type=MESH)

        for herald, mine in zip(heralds, serves):
            @pl.when(functools.reduce(jnp.logical_and, [my_env != herald[1], mine, jnp.logical_not(is_root)]))
            def _(herald=herald):
                pl.semaphore_signal(barrier, inc=1, device_id=at(herald), device_id_type=MESH)


        @pl.when(is_root)
        def _():
            def greet(k, state):
                for t in range(num_tm):
                    pl.semaphore_signal(
                        barrier, inc=1, device_id=at((t, lax.rem(my_env + k, num_env))), device_id_type=MESH
                    )
                return state

            lax.fori_loop(1, num_env, greet, 0)

        def link_copy(peer):
            return pltpu.make_async_remote_copy(
                src_ref=out.at[:, pl.ds(0, 2)], dst_ref=links.at[me, :, pl.ds(0, 2)],
                send_sem=load_sem.at[0], recv_sem=link_sem.at[0],
                device_id={"tm": peer}, device_id_type=MESH,
            )

        def root_copy(root, role, g):
            first, count = groups[g]
            rows = pl.ds(*span(role, g))
            return pltpu.make_async_remote_copy(
                src_ref=out.at[pl.ds(first, count), rows],
                dst_ref=table.at[me, pl.ds(first, count), rows, my_env],
                send_sem=load_sem.at[0], recv_sem=root_sem.at[0 if g < len(groups) - 1 else 1],
                device_id=at(root), device_id_type=MESH,
            )

        peers = [lax.rem(me + k, num_tm) for k in range(1, num_tm)]

        def send_block(devices, parts):
            for role in range(3):
                @pl.when(roles[role])
                def _(role=role):
                    for root in devices:
                        if role_of(root[0]) != role:
                            for g in parts:
                                root_copy(root, role, g).start()
                        else:
                            @pl.when(jnp.logical_not(here(root)))
                            def _(root=root):
                                for g in parts:
                                    root_copy(root, role, g).start()

        with scope("ldw00"):
            pending(load_sem.at[0], 3 * chunks + 3 * (seg_rows // pieces[0]) * SEGMENTS).wait_recv()
        inv_trace = 1.0 / (1.0 - 1.0 / params[2])
        discount = 1.0 - 1.0 / params[1]
        rate_all = discount * (1.0 - 1.0 / params[2])
        top = me == num_tm - 1
        ends = jnp.where(top, params[0] * inv_trace, 0.0)
        open_end = jnp.where(top, 0.0, 1.0)

        own = []
        early = max(chunks - 2, 0)
        zero = jnp.zeros((SEGMENTS, LANES), jnp.float32)
        total, squares = zero, zero
        for j in range(chunks):
            spread = lambda x: jnp.broadcast_to(x[:, j * LANES:(j + 1) * LANES], zero.shape)
            disc, rate, itr, end = spread(discount), spread(rate_all), spread(inv_trace), spread(ends)

            def steps(i, state, last_row, j=j, disc=disc, rate=rate):
                b, p, nv, s1, s2, s3, s4, s5 = state
                for u in range(min(STEPS_UNROLLED, size)):
                    r = last_row - (i * STEPS_UNROLLED + u)
                    v = val[j, r]
                    live = flg[j, r] == 0
                    d = jnp.where(live, disc, 0.0)
                    g = jnp.where(live, rate, 0.0)
                    b = (rew[j, r] - v + d * nv) + g * b
                    p = g * p
                    nv = v
                    base[j, r] = b
                    prop[j, r] = p
                    s1, s2, s3, s4, s5 = s1 + b, s2 + p, s3 + b * b, s4 + b * p, s5 + p * p
                return b, p, nv, s1, s2, s3, s4, s5

            state = (zero, zero + 1.0, zero) + (zero,) * 5
            size = seg_rows // pieces[j]
            for h in range(pieces[j]):
                if j == early and h == 0:
                    with scope("barw"):
                        far = sum(jnp.where(my_env == env, 0, 1) for _, env in roots)
                        for herald, devices in zip(heralds, told):
                            answers = sum(d[1] != herald[1] and d not in roots for d in devices)
                            far += jnp.where(here(herald), answers, 0)
                        pl.semaphore_wait(barrier, num_tm - 1 + far)
                    if len(groups) > 2:
                        with scope("send0"):
                            send_block(silent, [0])
                if j == last and h == pieces[j] - 1 and len(groups) > 2:
                    with scope("sendm"):
                        send_block(silent[:1], [1])
                if j + h:
                    with scope(f"ldw{j}{h}"):
                        pending(load_sem.at[at_piece[j] + h], 3 * size * SEGMENTS).wait_recv()
                with scope(f"scan{j}{h}"):
                    scan = functools.partial(steps, last_row=seg_rows - 1 - h * size)
                    state = lax.fori_loop(0, max(size // STEPS_UNROLLED, 1), scan, state)
            b, p, v, s1, s2, s3, s4, s5 = state
            x, a = b + v * itr, p
            for d in (1, 2, 4):
                x_next, a_next = shifted(x, d, 0.0), shifted(a, d, 1.0)
                x, a = x + a * x_next, a * a_next
            y, z = shifted(x, 1, 0.0), shifted(a, 1, 1.0)
            y, z = y + z * end, z * open_end
            own.append((y, z))
            total += s1 + s2 * y
            squares += s3 + y * (2.0 * s4 + s5 * y)
            out[j, 0:1, :] = a[0:1]
            out[j, 1:2, :] = x[0:1] + a[0:1] * end[0:1]
            for k, part in enumerate((s2 * z, (s4 + s5 * y) * z, s5 * z * z)):
                out[j, sums_row(j) + k:sums_row(j) + k + 1, :] = jnp.sum(part, axis=0, keepdims=True)
            if j == last:
                out[j, 2:3, :] = jnp.sum(total, axis=0, keepdims=True)
                out[j, 3:4, :] = jnp.sum(squares, axis=0, keepdims=True)
        with scope("send1"):
            late = range(1 if len(groups) > 2 else 0, len(groups))
            send_block(silent[:1], late[1:] if len(groups) > 2 else late)
            send_block(silent[1:], late)
        with scope("send2"):
            send_block(heralds, range(len(groups)))
            for peer in peers:
                link_copy(peer).start()

        with scope("linkw"):
            pending(link_sem.at[0], 2 * chunks * (num_tm - 1)).wait_recv()

        for j in range(chunks):
            y, z = own[j]
            carry = jnp.zeros((1, LANES), jnp.float32)
            mine = carry
            for t in range(num_tm - 1, 0, -1):
                carry = links[t, j, 1:2, :] + links[t, j, 0:1, :] * carry if t < num_tm - 1 else links[t, j, 1:2, :]
                mine = jnp.where(me == t - 1, carry, mine)
            c = y + z * jnp.where(top, 0.0, mine)

            def finish(i, state, j=j, c=c):
                for u in range(STEPS_UNROLLED):
                    r = i * STEPS_UNROLLED + u
                    rows = pl.ds(r, SEGMENTS, stride=pitch)
                    adv = base[j, r] + prop[j, r] * c
                    adv_ref[j, rows, :] = adv
                    ret_ref[j, rows, :] = adv + val[j, r]
                return state

            with scope(f"fin{j}"):
                lax.fori_loop(0, seg_rows // STEPS_UNROLLED, finish, 0)

        with scope("sendw"):
            for role in range(3):
                block = sum(sent(role, g) for g in range(len(groups)))

                @pl.when(jnp.logical_and(roles[role], is_root))
                def _(block=block):
                    pending(load_sem.at[0], link_rows + (len(roots) - 1) * block).wait_send()

                @pl.when(jnp.logical_and(roles[role], jnp.logical_not(is_root)))
                def _(block=block):
                    pending(load_sem.at[0], link_rows + len(roots) * block).wait_send()

    pl.run_scoped(scan_and_send, pltpu.SemaphoreType.DMA((sum(load_pieces(chunks)),)))

    def news_copy(t, e):
        return pltpu.make_async_remote_copy(
            src_ref=news.at[pl.ds(0, 2)], dst_ref=news.at[pl.ds(0, 2)],
            send_sem=link_sem.at[0], recv_sem=root_sem.at[0],
            device_id=at((t, e)), device_id_type=MESH,
        )

    @pl.when(is_root)
    def _():
        for j in range(chunks):
            for r in range(sums_row(j) + 3):
                table[me, j, r, pl.ds(my_env, 1), :] = out[j, r:r + 1, :]
        sums = [jnp.zeros((num_env, LANES), jnp.float32)] * 2
        for stage, parts in enumerate((range(len(groups) - 1), [len(groups) - 1])):
            with scope(f"rootw{stage}"):
                due = [sum(sent(role, g) for g in parts) for role in range(3)]
                everyone = num_env * sum(due[role_of(t)] for t in range(num_tm))
                for role in sorted({role_of(root[0]) for root in roots}):
                    if everyone:
                        @pl.when(roles[role])
                        def _(role=role):
                            pending(root_sem.at[stage], everyone - due[role], table).wait_recv()
            for j in [j for g in parts for j in range(groups[g][0], sum(groups[g]))]:
                first_sum = sums_row(j)
                carry = table[num_tm - 1, j, 1]
                for t in range(num_tm - 2, -1, -1):
                    sums[0] += table[t, j, first_sum] * carry
                    sums[1] += carry * (2.0 * table[t, j, first_sum + 1] + table[t, j, first_sum + 2] * carry)
                    if t:
                        carry = table[t, j, 1] + table[t, j, 0] * carry
        for t in range(num_tm):
            for k in range(2):
                sums[k] += table[t, last, 2 + k]
        for k in range(2):
            news[k:k + 1, :] = jnp.sum(sums[k], axis=0, keepdims=True)

    for herald, devices in zip(heralds, told):
        @pl.when(here(herald))
        def _(herald=herald, devices=devices):
            listeners = [d for d in devices if d not in roots]
            with scope("newsend"):
                for t, e in listeners:
                    if e == 0 or e == herald[1]:
                        news_copy(t, e).start()

                def tell(k, state):
                    e = jnp.where(k < herald[1], k, k + 1)
                    for t in sorted({t for t, _ in devices}):
                        news_copy(t, e).start()
                    return state

                lax.fori_loop(1, num_env - 1, tell, 0)
            with scope("newsw"):
                pending(link_sem.at[0], 2 * len(listeners)).wait_send()

    @pl.when(jnp.logical_not(is_root))
    def _():
        with scope("newsr"):
            pending(root_sem.at[0], 2).wait_recv()

    stats_ref[0:2, :] = news[0:2, :]


def write_kernel(cells, *refs):
    pl.run_scoped(functools.partial(write, cells, *refs), pltpu.SemaphoreType.DMA((2,)))


def write(cells, adv_ref, ret_ref, stats_ref, norm_hbm, ret_hbm, norm, sem):
    seg_rows = norm_hbm.shape[1]
    chunks = adv_ref.shape[0]
    pitch = seg_rows + PAD

    def out_copy(j, src, hbm, k):
        return pltpu.make_async_copy(
            src.at[j].reshape(SEGMENTS, pitch, LANES).at[:, pl.ds(0, seg_rows), :],
            hbm.at[:, :, pl.ds(j * LANES, LANES)],
            sem.at[k],
        )

    for j in range(chunks):
        out_copy(j, ret_ref, ret_hbm, 1).start()
    moments = jnp.sum(stats_ref[0:2, :], axis=1, keepdims=True) * (1.0 / cells)
    mean = moments[0:1]
    scale = lax.rsqrt(moments[1:2] - mean * mean + 1.0)
    mean = jnp.broadcast_to(mean, (8, LANES))
    scale = jnp.broadcast_to(scale, (8, LANES))
    for j in range(chunks):
        for s in range(SEGMENTS):
            for r in range(0, seg_rows, 8):
                at = pl.ds(s * pitch + r, 8)
                norm[j, at, :] = (adv_ref[j, at, :] - mean) * scale
        out_copy(j, norm, norm_hbm, 0).start()
    pltpu.make_async_copy(ret_hbm, ret_hbm, sem.at[1]).wait()
    pltpu.make_async_copy(norm_hbm, norm_hbm, sem.at[0]).wait()


def local(num_tm, num_env, rewards, values, done_flags, bootstrap, discount_horizon, trace_horizon):
    steps, width = rewards.shape
    seg_rows, chunks = steps // SEGMENTS, width // LANES
    pitch = seg_rows + PAD
    split = lambda x: x.reshape(SEGMENTS, seg_rows, width)
    row = lambda x: x.reshape(1, width)
    padded = (chunks, SEGMENTS * pitch, LANES)
    tiles = (chunks, seg_rows, SEGMENTS, LANES)
    hbm = pl.BlockSpec(memory_space=pltpu.HBM)
    vmem = pl.BlockSpec(memory_space=pltpu.VMEM)
    f32 = jnp.float32
    handed = 4 * (2 * chunks * SEGMENTS * pitch + 8) * LANES
    adv, ret, stats = pl.pallas_call(
        functools.partial(exchange_kernel, num_tm, num_env),
        out_shape=(pltpu.VMEM(padded, f32), pltpu.VMEM(padded, f32), pltpu.VMEM((8, LANES), f32)),
        in_specs=[hbm] * 6,
        out_specs=(vmem, vmem, vmem),
        scratch_shapes=[
            pltpu.VMEM(tiles, f32),
            pltpu.VMEM(tiles, f32),
            pltpu.VMEM(tiles, jnp.int32),
            pltpu.VMEM((3, 1, width), f32),
            pltpu.VMEM(tiles, f32),
            pltpu.VMEM(tiles, f32),
            pltpu.VMEM((chunks, 8, LANES), f32),
            pltpu.VMEM((num_tm, chunks, 8, LANES), f32),
            pltpu.VMEM((num_tm, chunks, ROWS, num_env, LANES), f32),
            pltpu.VMEM((8, LANES), f32),
            pltpu.SemaphoreType.DMA((1,)),
            pltpu.SemaphoreType.DMA((2,)),
        ],
        compiler_params=pltpu.CompilerParams(collective_id=0, has_side_effects=True, vmem_limit_bytes=VMEM_BYTES - handed),
    )(split(rewards), split(values), split(done_flags), row(bootstrap), row(discount_horizon), row(trace_horizon))
    norm_advantage, return_target = pl.pallas_call(
        functools.partial(write_kernel, float(steps * width * num_tm * num_env)),
        out_shape=(jax.ShapeDtypeStruct((SEGMENTS, seg_rows, width), f32),) * 2,
        in_specs=[vmem] * 3,
        out_specs=(hbm, hbm),
        scratch_shapes=[pltpu.VMEM(padded, f32)],
        compiler_params=pltpu.CompilerParams(vmem_limit_bytes=8 * 2**20),
    )(*(pltpu.with_memory_space_constraint(x, pltpu.VMEM) for x in (adv, ret, stats)))
    return norm_advantage.reshape(steps, width), return_target.reshape(steps, width)


def solution(mesh):
    placed = (P("tm", "env"), P("tm", "env"), P("tm", "env"), P("env"), P("env"), P("env"))
    return jax.shard_map(
        functools.partial(local, mesh.shape["tm"], mesh.shape["env"]),
        mesh=mesh,
        in_specs=placed,
        out_specs=(P("tm", "env"), P("tm", "env")),
        check_vma=False,
    )
```

```python
import functools

import jax
import jax.numpy as jnp
from jax import lax
from jax.experimental import pallas as pl
from jax.experimental.pallas import tpu as pltpu
from jax.sharding import PartitionSpec as P

MESH = pl.DeviceIdType.MESH
SEGMENTS = 8
LANES = 128
PAD = 8
STEPS_UNROLLED = 64
FINISH_UNROLLED = 16
VMEM_BYTES = 67043328
ROWS = 7
scope = jax.named_scope


def shifted(x, distance, fill):
    rows = lax.broadcasted_iota(jnp.int32, x.shape, 0)
    moved = pltpu.roll(x, SEGMENTS - distance, 0)
    return jnp.where(rows < SEGMENTS - distance, moved, fill)


def load_pieces(chunks):
    return [1] * (chunks - 1) + [2]


def send_groups(chunks):
    cuts = sorted({0, max(chunks - 2, 0), chunks - 1})
    return tuple((a, b - a) for a, b in zip(cuts, cuts[1:] + [chunks]))


def exchange_kernel(
    num_tm, num_env,
    rewards_hbm, values_hbm, flags_hbm, boot_hbm, disc_hbm, trace_hbm,
    adv_ref, ret_ref, stats_ref,
    rew, val, flg, params, out, links, table, news,
    link_sem, root_sem,
):
    me = lax.axis_index("tm")
    my_env = lax.axis_index("env")
    seg_rows, width = rewards_hbm.shape[1], rewards_hbm.shape[2]
    chunks = width // LANES
    pitch = seg_rows + PAD
    groups = send_groups(chunks)
    last = chunks - 1
    pair = 2 if num_tm % 2 == 0 else 1
    others = num_tm * num_env - 1

    silent = [(t, 0) for t in range(pair)]
    middle = num_env // 2 - 1
    heralds = [(num_tm - 1, middle), (pair - 1, middle)]
    if num_tm == pair:
        heralds = heralds[1:]
    roots = silent + heralds
    told = [
        [(t, e) for e in range(num_env) for t in range(pair, num_tm)],
        [(t, e) for e in range(1, num_env) for t in range(pair)],
    ][-len(heralds):]

    def here(device):
        return jnp.logical_and(me == device[0], my_env == device[1])

    is_root = functools.reduce(jnp.logical_or, [here(r) for r in roots])
    serves = [me >= pair, me < pair][-len(heralds):]

    def at(device):
        return {"tm": device[0], "env": device[1]}

    def rows_of(ref, n):
        count = 1
        for d in ref.shape[:-1]:
            count *= d
        return ref.reshape(count, LANES).at[pl.ds(0, n)]

    def pending(sem, n, ref=rew):
        part = rows_of(ref, n)
        return pltpu.make_async_remote_copy(
            src_ref=part, dst_ref=part, send_sem=sem, recv_sem=sem,
            device_id={"tm": lax.rem(me + 1, num_tm)}, device_id_type=MESH,
        )

    def sums_row(j):
        return 4 if j == chunks - 1 else 2

    def role_of(t):
        return 2 if t == num_tm - 1 else min(t, 1)

    def span(role, g):
        after = sums_row(groups[g][0] + groups[g][1] - 1)
        return ((2, after + 1), (0, after + 3), (1, after - 1))[role]

    def sent(role, g):
        return groups[g][1] * span(role, g)[1]

    roles = [me == 0, jnp.logical_and(me > 0, me < num_tm - 1), me == num_tm - 1]

    link_rows = 2 * chunks * (num_tm - 1)

    def scan_and_send(load_sem):
        pieces = load_pieces(chunks)
        at_piece = [sum(pieces[:j]) for j in range(chunks)]

        def load(j):
            size = seg_rows // pieces[j]
            for h in range(pieces[j]):
                rows = pl.ds((pieces[j] - 1 - h) * size, size)
                for s in range(SEGMENTS):
                    for hbm, vmem in ((rewards_hbm, rew), (values_hbm, val), (flags_hbm, flg)):
                        pltpu.make_async_copy(
                            hbm.at[s, rows, pl.ds(j * LANES, LANES)], vmem.at[j, rows, s], load_sem.at[at_piece[j] + h]
                        ).start()

        load(0)
        for a, hbm in enumerate((boot_hbm, disc_hbm, trace_hbm)):
            pltpu.make_async_copy(hbm, params.at[a], load_sem.at[0]).start()
        for j in range(1, chunks):
            load(j)
        barrier = pltpu.get_barrier_semaphore()
        for k in range(1, num_tm):
            pl.semaphore_signal(barrier, inc=1, device_id={"tm": lax.rem(me + k, num_tm)}, device_id_type=MESH)

        for herald, mine in zip(heralds, serves):
            @pl.when(functools.reduce(jnp.logical_and, [my_env != herald[1], mine, jnp.logical_not(is_root)]))
            def _(herald=herald):
                pl.semaphore_signal(barrier, inc=1, device_id=at(herald), device_id_type=MESH)


        @pl.when(is_root)
        def _():
            def greet(k, state):
                for t in range(num_tm):
                    pl.semaphore_signal(
                        barrier, inc=1, device_id=at((t, lax.rem(my_env + k, num_env))), device_id_type=MESH
                    )
                return state

            lax.fori_loop(1, num_env, greet, 0)

        def link_copy(peer):
            return pltpu.make_async_remote_copy(
                src_ref=out.at[:, pl.ds(0, 2)], dst_ref=links.at[me, :, pl.ds(0, 2)],
                send_sem=load_sem.at[0], recv_sem=link_sem.at[0],
                device_id={"tm": peer}, device_id_type=MESH,
            )

        def root_copy(root, role, g):
            first, count = groups[g]
            rows = pl.ds(*span(role, g))
            return pltpu.make_async_remote_copy(
                src_ref=out.at[pl.ds(first, count), rows],
                dst_ref=table.at[me, pl.ds(first, count), rows, my_env],
                send_sem=load_sem.at[0], recv_sem=root_sem.at[0 if g < len(groups) - 1 else 1],
                device_id=at(root), device_id_type=MESH,
            )

        peers = [lax.rem(me + k, num_tm) for k in range(1, num_tm)]

        def send_block(devices, parts):
            for role in range(3):
                @pl.when(roles[role])
                def _(role=role):
                    for root in devices:
                        if role_of(root[0]) != role:
                            for g in parts:
                                root_copy(root, role, g).start()
                        else:
                            @pl.when(jnp.logical_not(here(root)))
                            def _(root=root):
                                for g in parts:
                                    root_copy(root, role, g).start()

        with scope("ldw00"):
            pending(load_sem.at[0], 3 * chunks + 3 * (seg_rows // pieces[0]) * SEGMENTS).wait_recv()
        inv_trace = 1.0 / (1.0 - 1.0 / params[2])
        discount = 1.0 - 1.0 / params[1]
        rate_all = discount * (1.0 - 1.0 / params[2])
        top = me == num_tm - 1
        ends = jnp.where(top, params[0] * inv_trace, 0.0)
        open_end = jnp.where(top, 0.0, 1.0)

        def spread(x, j):
            return jnp.broadcast_to(x[:, j * LANES:(j + 1) * LANES], (SEGMENTS, LANES))

        own = []
        early = max(chunks - 2, 0)
        zero = jnp.zeros((SEGMENTS, LANES), jnp.float32)
        total, squares = zero, zero
        for j in range(chunks):
            disc, rate, itr, end = (spread(x, j) for x in (discount, rate_all, inv_trace, ends))

            def steps(i, state, last_row, j=j, disc=disc, rate=rate):
                b, p, nv, s1, s2, s3, s4, s5 = state
                for u in range(min(STEPS_UNROLLED, size)):
                    r = last_row - (i * STEPS_UNROLLED + u)
                    v = val[j, r]
                    live = flg[j, r] == 0
                    d = jnp.where(live, disc, 0.0)
                    g = jnp.where(live, rate, 0.0)
                    b = (rew[j, r] - v + d * nv) + g * b
                    p = g * p
                    nv = v
                    s1, s2, s3, s4, s5 = s1 + b, s2 + p, s3 + b * b, s4 + b * p, s5 + p * p
                return b, p, nv, s1, s2, s3, s4, s5

            state = (zero, zero + 1.0, zero) + (zero,) * 5
            size = seg_rows // pieces[j]
            for h in range(pieces[j]):
                if j == early and h == 0:
                    with scope("barw"):
                        far = sum(jnp.where(my_env == env, 0, 1) for _, env in roots)
                        for herald, devices in zip(heralds, told):
                            answers = sum(d[1] != herald[1] and d not in roots for d in devices)
                            far += jnp.where(here(herald), answers, 0)
                        pl.semaphore_wait(barrier, num_tm - 1 + far)
                    if len(groups) > 2:
                        with scope("send0"):
                            send_block(silent, [0])
                if j == last and h == pieces[j] - 1 and len(groups) > 2:
                    with scope("sendm"):
                        send_block(silent[:1], [1])
                if j + h:
                    with scope(f"ldw{j}{h}"):
                        pending(load_sem.at[at_piece[j] + h], 3 * size * SEGMENTS).wait_recv()
                with scope(f"scan{j}{h}"):
                    scan = functools.partial(steps, last_row=seg_rows - 1 - h * size)
                    state = lax.fori_loop(0, max(size // STEPS_UNROLLED, 1), scan, state)
            b, p, v, s1, s2, s3, s4, s5 = state
            x, a = b + v * itr, p
            for d in (1, 2, 4):
                x_next, a_next = shifted(x, d, 0.0), shifted(a, d, 1.0)
                x, a = x + a * x_next, a * a_next
            y, z = shifted(x, 1, 0.0), shifted(a, 1, 1.0)
            y, z = y + z * end, z * open_end
            own.append((y, z))
            total += s1 + s2 * y
            squares += s3 + y * (2.0 * s4 + s5 * y)
            out[j, 0:1, :] = a[0:1]
            out[j, 1:2, :] = x[0:1] + a[0:1] * end[0:1]
            for k, part in enumerate((s2 * z, (s4 + s5 * y) * z, s5 * z * z)):
                out[j, sums_row(j) + k:sums_row(j) + k + 1, :] = jnp.sum(part, axis=0, keepdims=True)
            if j == last:
                out[j, 2:3, :] = jnp.sum(total, axis=0, keepdims=True)
                out[j, 3:4, :] = jnp.sum(squares, axis=0, keepdims=True)
        with scope("send1"):
            late = range(1 if len(groups) > 2 else 0, len(groups))
            send_block(silent[:1], late[1:] if len(groups) > 2 else late)
            send_block(silent[1:], late)
        with scope("send2"):
            send_block(heralds, range(len(groups)))
            for peer in peers:
                link_copy(peer).start()

        with scope("linkw"):
            pending(link_sem.at[0], 2 * chunks * (num_tm - 1)).wait_recv()

        for j in range(chunks):
            y, z = own[j]
            carry = jnp.zeros((1, LANES), jnp.float32)
            mine = carry
            for t in range(num_tm - 1, 0, -1):
                carry = links[t, j, 1:2, :] + links[t, j, 0:1, :] * carry if t < num_tm - 1 else links[t, j, 1:2, :]
                mine = jnp.where(me == t - 1, carry, mine)
            c = y + z * jnp.where(top, 0.0, mine)

            disc, rate = spread(discount, j), spread(rate_all, j)

            def finish(i, state, j=j, disc=disc, rate=rate):
                adv, nv = state
                for u in range(FINISH_UNROLLED):
                    r = seg_rows - 1 - (i * FINISH_UNROLLED + u)
                    rows = pl.ds(r, SEGMENTS, stride=pitch)
                    v = val[j, r]
                    live = flg[j, r] == 0
                    d = jnp.where(live, disc, 0.0)
                    g = jnp.where(live, rate, 0.0)
                    adv = (rew[j, r] - v + d * nv) + g * adv
                    nv = v
                    adv_ref[j, rows, :] = adv
                    ret_ref[j, rows, :] = adv + v
                return adv, nv

            with scope(f"fin{j}"):
                lax.fori_loop(0, seg_rows // FINISH_UNROLLED, finish, (c, zero))

        with scope("sendw"):
            for role in range(3):
                block = sum(sent(role, g) for g in range(len(groups)))

                @pl.when(jnp.logical_and(roles[role], is_root))
                def _(block=block):
                    pending(load_sem.at[0], link_rows + (len(roots) - 1) * block).wait_send()

                @pl.when(jnp.logical_and(roles[role], jnp.logical_not(is_root)))
                def _(block=block):
                    pending(load_sem.at[0], link_rows + len(roots) * block).wait_send()

    pl.run_scoped(scan_and_send, pltpu.SemaphoreType.DMA((sum(load_pieces(chunks)),)))

    def news_copy(t, e):
        return pltpu.make_async_remote_copy(
            src_ref=news.at[pl.ds(0, 2)], dst_ref=news.at[pl.ds(0, 2)],
            send_sem=link_sem.at[0], recv_sem=root_sem.at[0],
            device_id=at((t, e)), device_id_type=MESH,
        )

    @pl.when(is_root)
    def _():
        for j in range(chunks):
            for r in range(sums_row(j) + 3):
                table[me, j, r, pl.ds(my_env, 1), :] = out[j, r:r + 1, :]
        sums = [jnp.zeros((num_env, LANES), jnp.float32)] * 2
        for stage, parts in enumerate((range(len(groups) - 1), [len(groups) - 1])):
            with scope(f"rootw{stage}"):
                due = [sum(sent(role, g) for g in parts) for role in range(3)]
                everyone = num_env * sum(due[role_of(t)] for t in range(num_tm))
                for role in sorted({role_of(root[0]) for root in roots}):
                    if everyone:
                        @pl.when(roles[role])
                        def _(role=role):
                            pending(root_sem.at[stage], everyone - due[role], table).wait_recv()
            for j in [j for g in parts for j in range(groups[g][0], sum(groups[g]))]:
                first_sum = sums_row(j)
                carry = table[num_tm - 1, j, 1]
                for t in range(num_tm - 2, -1, -1):
                    sums[0] += table[t, j, first_sum] * carry
                    sums[1] += carry * (2.0 * table[t, j, first_sum + 1] + table[t, j, first_sum + 2] * carry)
                    if t:
                        carry = table[t, j, 1] + table[t, j, 0] * carry
        for t in range(num_tm):
            for k in range(2):
                sums[k] += table[t, last, 2 + k]
        for k in range(2):
            news[k:k + 1, :] = jnp.sum(sums[k], axis=0, keepdims=True)

    for herald, devices in zip(heralds, told):
        @pl.when(here(herald))
        def _(herald=herald, devices=devices):
            listeners = [d for d in devices if d not in roots]
            with scope("newsend"):
                for t, e in listeners:
                    if e == 0 or e == herald[1]:
                        news_copy(t, e).start()

                def tell(k, state):
                    e = jnp.where(k < herald[1], k, k + 1)
                    for t in sorted({t for t, _ in devices}):
                        news_copy(t, e).start()
                    return state

                lax.fori_loop(1, num_env - 1, tell, 0)
            with scope("newsw"):
                pending(link_sem.at[0], 2 * len(listeners)).wait_send()

    @pl.when(jnp.logical_not(is_root))
    def _():
        with scope("newsr"):
            pending(root_sem.at[0], 2).wait_recv()

    stats_ref[0:2, :] = news[0:2, :]


def write_kernel(cells, *refs):
    pl.run_scoped(functools.partial(write, cells, *refs), pltpu.SemaphoreType.DMA((2,)))


def write(cells, adv_ref, ret_ref, stats_ref, norm_hbm, ret_hbm, norm, sem):
    seg_rows = norm_hbm.shape[1]
    chunks = adv_ref.shape[0]
    pitch = seg_rows + PAD

    def out_copy(j, src, hbm, k):
        return pltpu.make_async_copy(
            src.at[j].reshape(SEGMENTS, pitch, LANES).at[:, pl.ds(0, seg_rows), :],
            hbm.at[:, :, pl.ds(j * LANES, LANES)],
            sem.at[k],
        )

    for j in range(chunks):
        out_copy(j, ret_ref, ret_hbm, 1).start()
    moments = jnp.sum(stats_ref[0:2, :], axis=1, keepdims=True) * (1.0 / cells)
    mean = moments[0:1]
    scale = lax.rsqrt(moments[1:2] - mean * mean + 1.0)
    mean = jnp.broadcast_to(mean, (8, LANES))
    scale = jnp.broadcast_to(scale, (8, LANES))
    for j in range(chunks):
        for s in range(SEGMENTS):
            for r in range(0, seg_rows, 8):
                at = pl.ds(s * pitch + r, 8)
                norm[j, at, :] = (adv_ref[j, at, :] - mean) * scale
        out_copy(j, norm, norm_hbm, 0).start()
    pltpu.make_async_copy(ret_hbm, ret_hbm, sem.at[1]).wait()
    pltpu.make_async_copy(norm_hbm, norm_hbm, sem.at[0]).wait()


def local(num_tm, num_env, rewards, values, done_flags, bootstrap, discount_horizon, trace_horizon):
    steps, width = rewards.shape
    seg_rows, chunks = steps // SEGMENTS, width // LANES
    pitch = seg_rows + PAD
    split = lambda x: x.reshape(SEGMENTS, seg_rows, width)
    row = lambda x: x.reshape(1, width)
    padded = (chunks, SEGMENTS * pitch, LANES)
    tiles = (chunks, seg_rows, SEGMENTS, LANES)
    hbm = pl.BlockSpec(memory_space=pltpu.HBM)
    vmem = pl.BlockSpec(memory_space=pltpu.VMEM)
    f32 = jnp.float32
    handed = 4 * (2 * chunks * SEGMENTS * pitch + 8) * LANES
    adv, ret, stats = pl.pallas_call(
        functools.partial(exchange_kernel, num_tm, num_env),
        out_shape=(pltpu.VMEM(padded, f32), pltpu.VMEM(padded, f32), pltpu.VMEM((8, LANES), f32)),
        in_specs=[hbm] * 6,
        out_specs=(vmem, vmem, vmem),
        scratch_shapes=[
            pltpu.VMEM(tiles, f32),
            pltpu.VMEM(tiles, f32),
            pltpu.VMEM(tiles, jnp.int32),
            pltpu.VMEM((3, 1, width), f32),
            pltpu.VMEM((chunks, 8, LANES), f32),
            pltpu.VMEM((num_tm, chunks, 8, LANES), f32),
            pltpu.VMEM((num_tm, chunks, ROWS, num_env, LANES), f32),
            pltpu.VMEM((8, LANES), f32),
            pltpu.SemaphoreType.DMA((1,)),
            pltpu.SemaphoreType.DMA((2,)),
        ],
        compiler_params=pltpu.CompilerParams(collective_id=0, has_side_effects=True, vmem_limit_bytes=VMEM_BYTES - handed),
    )(split(rewards), split(values), split(done_flags), row(bootstrap), row(discount_horizon), row(trace_horizon))
    norm_advantage, return_target = pl.pallas_call(
        functools.partial(write_kernel, float(steps * width * num_tm * num_env)),
        out_shape=(jax.ShapeDtypeStruct((SEGMENTS, seg_rows, width), f32),) * 2,
        in_specs=[vmem] * 3,
        out_specs=(hbm, hbm),
        scratch_shapes=[pltpu.VMEM(padded, f32)],
        compiler_params=pltpu.CompilerParams(vmem_limit_bytes=8 * 2**20),
    )(*(pltpu.with_memory_space_constraint(x, pltpu.VMEM) for x in (adv, ret, stats)))
    return norm_advantage.reshape(steps, width), return_target.reshape(steps, width)


def solution(mesh):
    placed = (P("tm", "env"), P("tm", "env"), P("tm", "env"), P("env"), P("env"), P("env"))
    return jax.shard_map(
        functools.partial(local, mesh.shape["tm"], mesh.shape["env"]),
        mesh=mesh,
        in_specs=placed,
        out_specs=(P("tm", "env"), P("tm", "env")),
        check_vma=False,
    )
```

```python
import functools

import jax
import jax.numpy as jnp
from jax import lax
from jax.experimental import pallas as pl
from jax.experimental.pallas import tpu as pltpu
from jax.sharding import PartitionSpec as P

MESH = pl.DeviceIdType.MESH
SEGMENTS = 8
LANES = 128
PAD = 8
STEPS_UNROLLED = 64
VMEM_BYTES = 67043328
ROWS = 7
scope = jax.named_scope


def shifted(x, distance, fill):
    rows = lax.broadcasted_iota(jnp.int32, x.shape, 0)
    moved = pltpu.roll(x, SEGMENTS - distance, 0)
    return jnp.where(rows < SEGMENTS - distance, moved, fill)


def load_pieces(chunks):
    return [1] * (chunks - 1) + [2]


def send_groups(chunks):
    cuts = sorted({0, max(chunks - 2, 0), chunks - 1})
    return tuple((a, b - a) for a, b in zip(cuts, cuts[1:] + [chunks]))


def exchange_kernel(
    num_tm, num_env,
    rewards_hbm, values_hbm, flags_hbm, boot_hbm, disc_hbm, trace_hbm,
    adv_ref, ret_ref, stats_ref,
    rew, val, flg, params, base, prop, out, links, table, news,
    link_sem, root_sem,
):
    me = lax.axis_index("tm")
    my_env = lax.axis_index("env")
    seg_rows, width = rewards_hbm.shape[1], rewards_hbm.shape[2]
    chunks = width // LANES
    pitch = seg_rows + PAD
    groups = send_groups(chunks)
    last = chunks - 1
    pair = 2 if num_tm % 2 == 0 else 1
    others = num_tm * num_env - 1

    silent = [(t, 0) for t in range(pair)]
    middle = num_env // 2 - 1
    heralds = [(num_tm - 1, middle), (pair - 1, middle)]
    if num_tm == pair:
        heralds = heralds[1:]
    roots = silent + heralds
    told = [
        [(t, e) for e in range(num_env) for t in range(pair, num_tm)],
        [(t, e) for e in range(1, num_env) for t in range(pair)],
    ][-len(heralds):]

    def here(device):
        return jnp.logical_and(me == device[0], my_env == device[1])

    is_root = functools.reduce(jnp.logical_or, [here(r) for r in roots])
    serves = [me >= pair, me < pair][-len(heralds):]

    def at(device):
        return {"tm": device[0], "env": device[1]}

    def rows_of(ref, n):
        count = 1
        for d in ref.shape[:-1]:
            count *= d
        return ref.reshape(count, LANES).at[pl.ds(0, n)]

    def pending(sem, n, ref=base):
        part = rows_of(ref, n)
        return pltpu.make_async_remote_copy(
            src_ref=part, dst_ref=part, send_sem=sem, recv_sem=sem,
            device_id={"tm": lax.rem(me + 1, num_tm)}, device_id_type=MESH,
        )

    def sums_row(j):
        return 4 if j == chunks - 1 else 2

    def role_of(t):
        return 2 if t == num_tm - 1 else min(t, 1)

    def span(role, g):
        after = sums_row(groups[g][0] + groups[g][1] - 1)
        return ((2, after + 1), (0, after + 3), (1, after - 1))[role]

    def sent(role, g):
        return groups[g][1] * span(role, g)[1]

    roles = [me == 0, jnp.logical_and(me > 0, me < num_tm - 1), me == num_tm - 1]

    link_rows = 2 * chunks * (num_tm - 1)

    def scan_and_send(load_sem):
        pieces = load_pieces(chunks)
        at_piece = [sum(pieces[:j]) for j in range(chunks)]

        def load(j):
            size = seg_rows // pieces[j]
            for h in range(pieces[j]):
                rows = pl.ds((pieces[j] - 1 - h) * size, size)
                for s in range(SEGMENTS):
                    for hbm, vmem in ((rewards_hbm, rew), (values_hbm, val), (flags_hbm, flg)):
                        pltpu.make_async_copy(
                            hbm.at[s, rows, pl.ds(j * LANES, LANES)], vmem.at[j, rows, s], load_sem.at[at_piece[j] + h]
                        ).start()

        load(0)
        for a, hbm in enumerate((boot_hbm, disc_hbm, trace_hbm)):
            pltpu.make_async_copy(hbm, params.at[a], load_sem.at[0]).start()
        for j in range(1, chunks):
            load(j)
        barrier = pltpu.get_barrier_semaphore()
        for k in range(1, num_tm):
            pl.semaphore_signal(barrier, inc=1, device_id={"tm": lax.rem(me + k, num_tm)}, device_id_type=MESH)

        for herald, mine in zip(heralds, serves):
            @pl.when(functools.reduce(jnp.logical_and, [my_env != herald[1], mine, jnp.logical_not(is_root)]))
            def _(herald=herald):
                pl.semaphore_signal(barrier, inc=1, device_id=at(herald), device_id_type=MESH)


        @pl.when(is_root)
        def _():
            def greet(k, state):
                for t in range(num_tm):
                    pl.semaphore_signal(
                        barrier, inc=1, device_id=at((t, lax.rem(my_env + k, num_env))), device_id_type=MESH
                    )
                return state

            lax.fori_loop(1, num_env, greet, 0)

        def link_copy(peer):
            return pltpu.make_async_remote_copy(
                src_ref=out.at[:, pl.ds(0, 2)], dst_ref=links.at[me, :, pl.ds(0, 2)],
                send_sem=load_sem.at[0], recv_sem=link_sem.at[0],
                device_id={"tm": peer}, device_id_type=MESH,
            )

        def root_copy(root, role, g):
            first, count = groups[g]
            rows = pl.ds(*span(role, g))
            return pltpu.make_async_remote_copy(
                src_ref=out.at[pl.ds(first, count), rows],
                dst_ref=table.at[me, pl.ds(first, count), rows, my_env],
                send_sem=load_sem.at[0], recv_sem=root_sem.at[0 if g < len(groups) - 1 else 1],
                device_id=at(root), device_id_type=MESH,
            )

        peers = [lax.rem(me + k, num_tm) for k in range(1, num_tm)]

        def send_block(devices, parts):
            for role in range(3):
                @pl.when(roles[role])
                def _(role=role):
                    for root in devices:
                        if role_of(root[0]) != role:
                            for g in parts:
                                root_copy(root, role, g).start()
                        else:
                            @pl.when(jnp.logical_not(here(root)))
                            def _(root=root):
                                for g in parts:
                                    root_copy(root, role, g).start()

        with scope("ldw00"):
            pending(load_sem.at[0], 3 * chunks + 3 * (seg_rows // pieces[0]) * SEGMENTS).wait_recv()
        inv_trace = 1.0 / (1.0 - 1.0 / params[2])
        discount = 1.0 - 1.0 / params[1]
        rate_all = discount * (1.0 - 1.0 / params[2])
        top = me == num_tm - 1
        ends = jnp.where(top, params[0] * inv_trace, 0.0)
        open_end = jnp.where(top, 0.0, 1.0)

        own = []
        early = max(chunks - 2, 0)
        zero = jnp.zeros((SEGMENTS, LANES), jnp.float32)
        total, squares = zero, zero
        for j in range(chunks):
            spread = lambda x: jnp.broadcast_to(x[:, j * LANES:(j + 1) * LANES], zero.shape)
            disc, rate, itr, end = spread(discount), spread(rate_all), spread(inv_trace), spread(ends)

            def steps(i, state, last_row, j=j, disc=disc, rate=rate):
                b, p, nv, s1, s2, s3, s4, s5 = state
                for u in range(min(STEPS_UNROLLED, size)):
                    r = last_row - (i * STEPS_UNROLLED + u)
                    v = val[j, r]
                    live = flg[j, r] == 0
                    d = jnp.where(live, disc, 0.0)
                    g = jnp.where(live, rate, 0.0)
                    b = (rew[j, r] - v + d * nv) + g * b
                    p = g * p
                    nv = v
                    base[j, r] = b
                    prop[j, r] = p
                    s1, s2, s3, s4, s5 = s1 + b, s2 + p, s3 + b * b, s4 + b * p, s5 + p * p
                return b, p, nv, s1, s2, s3, s4, s5

            state = (zero, zero + 1.0, zero) + (zero,) * 5
            size = seg_rows // pieces[j]
            for h in range(pieces[j]):
                if j == early and h == 0:
                    with scope("barw"):
                        far = sum(jnp.where(my_env == env, 0, 1) for _, env in roots)
                        for herald, devices in zip(heralds, told):
                            answers = sum(d[1] != herald[1] and d not in roots for d in devices)
                            far += jnp.where(here(herald), answers, 0)
                        pl.semaphore_wait(barrier, num_tm - 1 + far)
                    if len(groups) > 2:
                        with scope("send0"):
                            send_block(silent, [0])
                if j == last and h == pieces[j] - 1 and len(groups) > 2:
                    with scope("sendm"):
                        send_block(silent[:1], [1])
                if j + h:
                    with scope(f"ldw{j}{h}"):
                        pending(load_sem.at[at_piece[j] + h], 3 * size * SEGMENTS).wait_recv()
                with scope(f"scan{j}{h}"):
                    scan = functools.partial(steps, last_row=seg_rows - 1 - h * size)
                    state = lax.fori_loop(0, max(size // STEPS_UNROLLED, 1), scan, state)
            b, p, v, s1, s2, s3, s4, s5 = state
            x, a = b + v * itr, p
            for d in (1, 2, 4):
                x_next, a_next = shifted(x, d, 0.0), shifted(a, d, 1.0)
                x, a = x + a * x_next, a * a_next
            y, z = shifted(x, 1, 0.0), shifted(a, 1, 1.0)
            y, z = y + z * end, z * open_end
            own.append((y, z))
            total += s1 + s2 * y
            squares += s3 + y * (2.0 * s4 + s5 * y)
            out[j, 0:1, :] = a[0:1]
            out[j, 1:2, :] = x[0:1] + a[0:1] * end[0:1]
            for k, part in enumerate((s2 * z, (s4 + s5 * y) * z, s5 * z * z)):
                out[j, sums_row(j) + k:sums_row(j) + k + 1, :] = jnp.sum(part, axis=0, keepdims=True)
            if j == last:
                out[j, 2:3, :] = jnp.sum(total, axis=0, keepdims=True)
                out[j, 3:4, :] = jnp.sum(squares, axis=0, keepdims=True)
        with scope("send1"):
            late = range(1 if len(groups) > 2 else 0, len(groups))
            send_block(silent[:1], late[1:] if len(groups) > 2 else late)
            send_block(silent[1:], late)
        with scope("send2"):
            send_block(heralds, range(len(groups)))
            for peer in peers:
                link_copy(peer).start()

        with scope("linkw"):
            pending(link_sem.at[0], 2 * chunks * (num_tm - 1)).wait_recv()

        for j in range(chunks):
            y, z = own[j]
            carry = jnp.zeros((1, LANES), jnp.float32)
            mine = carry
            for t in range(num_tm - 1, 0, -1):
                carry = links[t, j, 1:2, :] + links[t, j, 0:1, :] * carry if t < num_tm - 1 else links[t, j, 1:2, :]
                mine = jnp.where(me == t - 1, carry, mine)
            c = y + z * jnp.where(top, 0.0, mine)

            def finish(i, state, j=j, c=c):
                for u in range(STEPS_UNROLLED):
                    r = i * STEPS_UNROLLED + u
                    rows = pl.ds(r, SEGMENTS, stride=pitch)
                    adv = base[j, r] + prop[j, r] * c
                    adv_ref[j, rows, :] = adv
                    ret_ref[j, rows, :] = adv + val[j, r]
                return state

            with scope(f"fin{j}"):
                lax.fori_loop(0, seg_rows // STEPS_UNROLLED, finish, 0)

        with scope("sendw"):
            for role in range(3):
                block = sum(sent(role, g) for g in range(len(groups)))

                @pl.when(jnp.logical_and(roles[role], is_root))
                def _(block=block):
                    pending(load_sem.at[0], link_rows + (len(roots) - 1) * block).wait_send()

                @pl.when(jnp.logical_and(roles[role], jnp.logical_not(is_root)))
                def _(block=block):
                    pending(load_sem.at[0], link_rows + len(roots) * block).wait_send()

    pl.run_scoped(scan_and_send, pltpu.SemaphoreType.DMA((sum(load_pieces(chunks)),)))

    def news_copy(t, e):
        return pltpu.make_async_remote_copy(
            src_ref=news.at[pl.ds(0, 2)], dst_ref=news.at[pl.ds(0, 2)],
            send_sem=link_sem.at[0], recv_sem=root_sem.at[0],
            device_id=at((t, e)), device_id_type=MESH,
        )

    @pl.when(is_root)
    def _():
        for j in range(chunks):
            for r in range(sums_row(j) + 3):
                table[me, j, r, pl.ds(my_env, 1), :] = out[j, r:r + 1, :]
        sums = [jnp.zeros((num_env, LANES), jnp.float32)] * 2
        for stage, parts in enumerate((range(len(groups) - 1), [len(groups) - 1])):
            with scope(f"rootw{stage}"):
                due = [sum(sent(role, g) for g in parts) for role in range(3)]
                everyone = num_env * sum(due[role_of(t)] for t in range(num_tm))
                for role in sorted({role_of(root[0]) for root in roots}):
                    if everyone:
                        @pl.when(roles[role])
                        def _(role=role):
                            pending(root_sem.at[stage], everyone - due[role], table).wait_recv()
            for j in [j for g in parts for j in range(groups[g][0], sum(groups[g]))]:
                first_sum = sums_row(j)
                carry = table[num_tm - 1, j, 1]
                for t in range(num_tm - 2, -1, -1):
                    sums[0] += table[t, j, first_sum] * carry
                    sums[1] += carry * (2.0 * table[t, j, first_sum + 1] + table[t, j, first_sum + 2] * carry)
                    if t:
                        carry = table[t, j, 1] + table[t, j, 0] * carry
        for t in range(num_tm):
            for k in range(2):
                sums[k] += table[t, last, 2 + k]
        for k in range(2):
            part = jnp.sum(sums[k], axis=0, keepdims=True)
            stats_ref[k:k + 1, :] = part
            news[k:k + 1, :] = part

    for herald, devices in zip(heralds, told):
        @pl.when(here(herald))
        def _(herald=herald, devices=devices):
            listeners = [d for d in devices if d not in roots]
            with scope("newsend"):
                for t, e in listeners:
                    if e == 0 or e == herald[1]:
                        news_copy(t, e).start()

                def tell(k, state):
                    e = jnp.where(k < herald[1], k, k + 1)
                    for t in sorted({t for t, _ in devices}):
                        news_copy(t, e).start()
                    return state

                lax.fori_loop(1, num_env - 1, tell, 0)
            with scope("newsw"):
                pending(link_sem.at[0], 2 * len(listeners)).wait_send()

    @pl.when(jnp.logical_not(is_root))
    def _():
        with scope("newsr"):
            pending(root_sem.at[0], 2).wait_recv()
        stats_ref[0:2, :] = news[0:2, :]


def write_kernel(cells, *refs):
    pl.run_scoped(functools.partial(write, cells, *refs), pltpu.SemaphoreType.DMA((2,)))


def write(cells, adv_ref, ret_ref, stats_ref, norm_hbm, ret_hbm, norm, sem):
    seg_rows = norm_hbm.shape[1]
    chunks = adv_ref.shape[0]
    pitch = seg_rows + PAD

    def out_copy(j, src, hbm, k):
        return pltpu.make_async_copy(
            src.at[j].reshape(SEGMENTS, pitch, LANES).at[:, pl.ds(0, seg_rows), :],
            hbm.at[:, :, pl.ds(j * LANES, LANES)],
            sem.at[k],
        )

    for j in range(chunks):
        out_copy(j, ret_ref, ret_hbm, 1).start()
    moments = jnp.sum(stats_ref[0:2, :], axis=1, keepdims=True) * (1.0 / cells)
    mean = moments[0:1]
    scale = lax.rsqrt(moments[1:2] - mean * mean + 1.0)
    mean = jnp.broadcast_to(mean, (8, LANES))
    scale = jnp.broadcast_to(scale, (8, LANES))
    for j in range(chunks):
        for s in range(SEGMENTS):
            for r in range(0, seg_rows, 8):
                at = pl.ds(s * pitch + r, 8)
                norm[j, at, :] = (adv_ref[j, at, :] - mean) * scale
        out_copy(j, norm, norm_hbm, 0).start()
    pltpu.make_async_copy(ret_hbm, ret_hbm, sem.at[1]).wait()
    pltpu.make_async_copy(norm_hbm, norm_hbm, sem.at[0]).wait()


def local(num_tm, num_env, rewards, values, done_flags, bootstrap, discount_horizon, trace_horizon):
    steps, width = rewards.shape
    seg_rows, chunks = steps // SEGMENTS, width // LANES
    pitch = seg_rows + PAD
    split = lambda x: x.reshape(SEGMENTS, seg_rows, width)
    row = lambda x: x.reshape(1, width)
    padded = (chunks, SEGMENTS * pitch, LANES)
    tiles = (chunks, seg_rows, SEGMENTS, LANES)
    hbm = pl.BlockSpec(memory_space=pltpu.HBM)
    vmem = pl.BlockSpec(memory_space=pltpu.VMEM)
    f32 = jnp.float32
    handed = 4 * (2 * chunks * SEGMENTS * pitch + 8) * LANES
    adv, ret, stats = pl.pallas_call(
        functools.partial(exchange_kernel, num_tm, num_env),
        out_shape=(pltpu.VMEM(padded, f32), pltpu.VMEM(padded, f32), pltpu.VMEM((8, LANES), f32)),
        in_specs=[hbm] * 6,
        out_specs=(vmem, vmem, vmem),
        scratch_shapes=[
            pltpu.VMEM(tiles, f32),
            pltpu.VMEM(tiles, f32),
            pltpu.VMEM(tiles, jnp.int32),
            pltpu.VMEM((3, 1, width), f32),
            pltpu.VMEM(tiles, f32),
            pltpu.VMEM(tiles, f32),
            pltpu.VMEM((chunks, 8, LANES), f32),
            pltpu.VMEM((num_tm, chunks, 8, LANES), f32),
            pltpu.VMEM((num_tm, chunks, ROWS, num_env, LANES), f32),
            pltpu.VMEM((8, LANES), f32),
            pltpu.SemaphoreType.DMA((1,)),
            pltpu.SemaphoreType.DMA((2,)),
        ],
        compiler_params=pltpu.CompilerParams(collective_id=0, has_side_effects=True, vmem_limit_bytes=VMEM_BYTES - handed),
    )(split(rewards), split(values), split(done_flags), row(bootstrap), row(discount_horizon), row(trace_horizon))
    norm_advantage, return_target = pl.pallas_call(
        functools.partial(write_kernel, float(steps * width * num_tm * num_env)),
        out_shape=(jax.ShapeDtypeStruct((SEGMENTS, seg_rows, width), f32),) * 2,
        in_specs=[vmem] * 3,
        out_specs=(hbm, hbm),
        scratch_shapes=[pltpu.VMEM(padded, f32)],
        compiler_params=pltpu.CompilerParams(vmem_limit_bytes=8 * 2**20),
    )(*(pltpu.with_memory_space_constraint(x, pltpu.VMEM) for x in (adv, ret, stats)))
    return norm_advantage.reshape(steps, width), return_target.reshape(steps, width)


def solution(mesh):
    placed = (P("tm", "env"), P("tm", "env"), P("tm", "env"), P("env"), P("env"), P("env"))
    return jax.shard_map(
        functools.partial(local, mesh.shape["tm"], mesh.shape["env"]),
        mesh=mesh,
        in_specs=placed,
        out_specs=(P("tm", "env"), P("tm", "env")),
        check_vma=False,
    )
```

```python
import functools

import jax
import jax.numpy as jnp
from jax import lax
from jax.experimental import pallas as pl
from jax.experimental.pallas import tpu as pltpu
from jax.sharding import PartitionSpec as P

MESH = pl.DeviceIdType.MESH
SEGMENTS = 8
LANES = 128
PAD = 8
STEPS_UNROLLED = 64
VMEM_BYTES = 67043328
ROWS = 7
scope = jax.named_scope


def shifted(x, distance, fill):
    rows = lax.broadcasted_iota(jnp.int32, x.shape, 0)
    moved = pltpu.roll(x, SEGMENTS - distance, 0)
    return jnp.where(rows < SEGMENTS - distance, moved, fill)


def load_pieces(chunks):
    return [1] * (chunks - 1) + [2]


def send_groups(chunks):
    cuts = sorted({0, max(chunks - 2, 0), chunks - 1})
    return tuple((a, b - a) for a, b in zip(cuts, cuts[1:] + [chunks]))


def exchange_kernel(
    num_tm, num_env,
    rewards_hbm, values_hbm, flags_hbm, boot_hbm, disc_hbm, trace_hbm,
    adv_ref, ret_ref, stats_ref,
    rew, val, flg, params, base, prop, out, links, table, news,
    link_sem, root_sem,
):
    me = lax.axis_index("tm")
    my_env = lax.axis_index("env")
    seg_rows, width = rewards_hbm.shape[1], rewards_hbm.shape[2]
    chunks = width // LANES
    pitch = seg_rows + PAD
    groups = send_groups(chunks)
    last = chunks - 1
    pair = 2 if num_tm % 2 == 0 else 1
    others = num_tm * num_env - 1

    silent = [(t, 0) for t in range(pair)]
    middle = num_env // 2 - 1
    heralds = [(num_tm - 1, middle), (pair - 1, middle)]
    if num_tm == pair:
        heralds = heralds[1:]
    roots = silent + heralds
    told = [
        [(t, e) for e in range(num_env) for t in range(pair, num_tm)],
        [(t, e) for e in range(1, num_env) for t in range(pair)],
    ][-len(heralds):]

    def here(device):
        return jnp.logical_and(me == device[0], my_env == device[1])

    is_root = functools.reduce(jnp.logical_or, [here(r) for r in roots])
    serves = [me >= pair, me < pair][-len(heralds):]

    def at(device):
        return {"tm": device[0], "env": device[1]}

    def rows_of(ref, n):
        count = 1
        for d in ref.shape[:-1]:
            count *= d
        return ref.reshape(count, LANES).at[pl.ds(0, n)]

    def pending(sem, n, ref=base):
        part = rows_of(ref, n)
        return pltpu.make_async_remote_copy(
            src_ref=part, dst_ref=part, send_sem=sem, recv_sem=sem,
            device_id={"tm": lax.rem(me + 1, num_tm)}, device_id_type=MESH,
        )

    def sums_row(j):
        return 4 if j == chunks - 1 else 2

    def role_of(t):
        return 2 if t == num_tm - 1 else min(t, 1)

    def span(role, g):
        after = sums_row(groups[g][0] + groups[g][1] - 1)
        return ((2, after + 1), (0, after + 3), (1, after - 1))[role]

    def sent(role, g):
        return groups[g][1] * span(role, g)[1]

    roles = [me == 0, jnp.logical_and(me > 0, me < num_tm - 1), me == num_tm - 1]

    link_rows = 2 * chunks * (num_tm - 1)

    def scan_and_send(load_sem):
        pieces = load_pieces(chunks)
        at_piece = [sum(pieces[:j]) for j in range(chunks)]

        def load(j):
            size = seg_rows // pieces[j]
            for h in range(pieces[j]):
                rows = pl.ds((pieces[j] - 1 - h) * size, size)
                for s in range(SEGMENTS):
                    for hbm, vmem in ((rewards_hbm, rew), (values_hbm, val), (flags_hbm, flg)):
                        pltpu.make_async_copy(
                            hbm.at[s, rows, pl.ds(j * LANES, LANES)], vmem.at[j, rows, s], load_sem.at[at_piece[j] + h]
                        ).start()

        load(0)
        for a, hbm in enumerate((boot_hbm, disc_hbm, trace_hbm)):
            pltpu.make_async_copy(hbm, params.at[a], load_sem.at[0]).start()
        for j in range(1, chunks):
            load(j)
        barrier = pltpu.get_barrier_semaphore()
        for k in range(1, num_tm):
            pl.semaphore_signal(barrier, inc=1, device_id={"tm": lax.rem(me + k, num_tm)}, device_id_type=MESH)

        for herald, mine in zip(heralds, serves):
            @pl.when(functools.reduce(jnp.logical_and, [my_env != herald[1], mine, jnp.logical_not(is_root)]))
            def _(herald=herald):
                pl.semaphore_signal(barrier, inc=1, device_id=at(herald), device_id_type=MESH)


        @pl.when(is_root)
        def _():
            def greet(k, state):
                for t in range(num_tm):
                    pl.semaphore_signal(
                        barrier, inc=1, device_id=at((t, lax.rem(my_env + k, num_env))), device_id_type=MESH
                    )
                return state

            lax.fori_loop(1, num_env, greet, 0)

        def link_copy(peer):
            return pltpu.make_async_remote_copy(
                src_ref=out.at[:, pl.ds(0, 2)], dst_ref=links.at[me, :, pl.ds(0, 2)],
                send_sem=load_sem.at[0], recv_sem=link_sem.at[0],
                device_id={"tm": peer}, device_id_type=MESH,
            )

        def root_copy(root, role, g):
            first, count = groups[g]
            rows = pl.ds(*span(role, g))
            return pltpu.make_async_remote_copy(
                src_ref=out.at[pl.ds(first, count), rows],
                dst_ref=table.at[me, pl.ds(first, count), rows, my_env],
                send_sem=load_sem.at[0], recv_sem=root_sem.at[0 if g < len(groups) - 1 else 1],
                device_id=at(root), device_id_type=MESH,
            )

        peers = [lax.rem(me + k, num_tm) for k in range(1, num_tm)]

        def send_block(devices, parts):
            for role in range(3):
                @pl.when(roles[role])
                def _(role=role):
                    for root in devices:
                        if role_of(root[0]) != role:
                            for g in parts:
                                root_copy(root, role, g).start()
                        else:
                            @pl.when(jnp.logical_not(here(root)))
                            def _(root=root):
                                for g in parts:
                                    root_copy(root, role, g).start()

        with scope("ldw00"):
            pending(load_sem.at[0], 3 * chunks + 3 * (seg_rows // pieces[0]) * SEGMENTS).wait_recv()
        inv_trace = 1.0 / (1.0 - 1.0 / params[2])
        discount = 1.0 - 1.0 / params[1]
        rate_all = discount * (1.0 - 1.0 / params[2])
        top = me == num_tm - 1
        ends = jnp.where(top, params[0] * inv_trace, 0.0)
        open_end = jnp.where(top, 0.0, 1.0)

        own = []
        early = max(chunks - 2, 0)
        zero = jnp.zeros((SEGMENTS, LANES), jnp.float32)
        total, squares = zero, zero
        for j in range(chunks):
            spread = lambda x: jnp.broadcast_to(x[:, j * LANES:(j + 1) * LANES], zero.shape)
            disc, rate, itr, end = spread(discount), spread(rate_all), spread(inv_trace), spread(ends)

            def steps(i, state, last_row, j=j, disc=disc, rate=rate):
                b, p, nv, s1, s2, s3, s4, s5 = state
                for u in range(min(STEPS_UNROLLED, size)):
                    r = last_row - (i * STEPS_UNROLLED + u)
                    v = val[j, r]
                    live = flg[j, r] == 0
                    d = jnp.where(live, disc, 0.0)
                    g = jnp.where(live, rate, 0.0)
                    b = (rew[j, r] - v + d * nv) + g * b
                    p = g * p
                    nv = v
                    base[j, r] = b
                    prop[j, r] = p
                    s1, s2, s3, s4, s5 = s1 + b, s2 + p, s3 + b * b, s4 + b * p, s5 + p * p
                return b, p, nv, s1, s2, s3, s4, s5

            state = (zero, zero + 1.0, zero) + (zero,) * 5
            size = seg_rows // pieces[j]
            for h in range(pieces[j]):
                if j == early and h == 0:
                    with scope("barw"):
                        far = sum(jnp.where(my_env == env, 0, 1) for _, env in roots)
                        for herald, devices in zip(heralds, told):
                            answers = sum(d[1] != herald[1] and d not in roots for d in devices)
                            far += jnp.where(here(herald), answers, 0)
                        pl.semaphore_wait(barrier, num_tm - 1 + far)
                    if len(groups) > 2:
                        with scope("send0"):
                            send_block(silent, [0])
                if j == last and h == pieces[j] - 1 and len(groups) > 2:
                    with scope("sendm"):
                        send_block(silent[:1], [1])
                if j + h:
                    with scope(f"ldw{j}{h}"):
                        pending(load_sem.at[at_piece[j] + h], 3 * size * SEGMENTS).wait_recv()
                with scope(f"scan{j}{h}"):
                    scan = functools.partial(steps, last_row=seg_rows - 1 - h * size)
                    state = lax.fori_loop(0, max(size // STEPS_UNROLLED, 1), scan, state)
            b, p, v, s1, s2, s3, s4, s5 = state
            x, a = b + v * itr, p
            for d in (1, 2, 4):
                x_next, a_next = shifted(x, d, 0.0), shifted(a, d, 1.0)
                x, a = x + a * x_next, a * a_next
            y, z = shifted(x, 1, 0.0), shifted(a, 1, 1.0)
            y, z = y + z * end, z * open_end
            own.append((y, z))
            total += s1 + s2 * y
            squares += s3 + y * (2.0 * s4 + s5 * y)
            out[j, 0:1, :] = a[0:1]
            out[j, 1:2, :] = x[0:1] + a[0:1] * end[0:1]
            for k, part in enumerate((s2 * z, (s4 + s5 * y) * z, s5 * z * z)):
                out[j, sums_row(j) + k:sums_row(j) + k + 1, :] = jnp.sum(part, axis=0, keepdims=True)
            if j == last:
                out[j, 2:3, :] = jnp.sum(total, axis=0, keepdims=True)
                out[j, 3:4, :] = jnp.sum(squares, axis=0, keepdims=True)
        with scope("send1"):
            late = range(1 if len(groups) > 2 else 0, len(groups))
            send_block(silent[:1], late[1:] if len(groups) > 2 else late)
            send_block(silent[1:], late)
        with scope("send2"):
            send_block(heralds, range(len(groups)))
            for peer in peers:
                link_copy(peer).start()

        with scope("linkw"):
            pending(link_sem.at[0], 2 * chunks * (num_tm - 1)).wait_recv()

        for j in range(chunks):
            y, z = own[j]
            carry = jnp.zeros((1, LANES), jnp.float32)
            mine = carry
            for t in range(num_tm - 1, 0, -1):
                carry = links[t, j, 1:2, :] + links[t, j, 0:1, :] * carry if t < num_tm - 1 else links[t, j, 1:2, :]
                mine = jnp.where(me == t - 1, carry, mine)
            c = y + z * jnp.where(top, 0.0, mine)

            def finish(i, state, j=j, c=c):
                for u in range(STEPS_UNROLLED):
                    r = i * STEPS_UNROLLED + u
                    rows = pl.ds(r, SEGMENTS, stride=pitch)
                    adv = base[j, r] + prop[j, r] * c
                    adv_ref[j, rows, :] = adv
                    ret_ref[j, rows, :] = adv + val[j, r]
                return state

            with scope(f"fin{j}"):
                lax.fori_loop(0, seg_rows // STEPS_UNROLLED, finish, 0)

        with scope("sendw"):
            for role in range(3):
                block = sum(sent(role, g) for g in range(len(groups)))

                @pl.when(jnp.logical_and(roles[role], is_root))
                def _(block=block):
                    pending(load_sem.at[0], link_rows + (len(roots) - 1) * block).wait_send()

                @pl.when(jnp.logical_and(roles[role], jnp.logical_not(is_root)))
                def _(block=block):
                    pending(load_sem.at[0], link_rows + len(roots) * block).wait_send()

    pl.run_scoped(scan_and_send, pltpu.SemaphoreType.DMA((sum(load_pieces(chunks)),)))

    def news_copy(t, e):
        return pltpu.make_async_remote_copy(
            src_ref=news.at[pl.ds(0, 2)], dst_ref=news.at[pl.ds(0, 2)],
            send_sem=link_sem.at[0], recv_sem=root_sem.at[0],
            device_id=at((t, e)), device_id_type=MESH,
        )

    @pl.when(is_root)
    def _():
        for j in range(chunks):
            for r in range(sums_row(j) + 3):
                table[me, j, r, pl.ds(my_env, 1), :] = out[j, r:r + 1, :]
        sums = [jnp.zeros((num_env, LANES), jnp.float32)] * 2
        for stage, parts in enumerate((range(len(groups) - 1), [len(groups) - 1])):
            with scope(f"rootw{stage}"):
                due = [sum(sent(role, g) for g in parts) for role in range(3)]
                everyone = num_env * sum(due[role_of(t)] for t in range(num_tm))
                for role in sorted({role_of(root[0]) for root in roots}):
                    if everyone:
                        @pl.when(roles[role])
                        def _(role=role):
                            pending(root_sem.at[stage], everyone - due[role], table).wait_recv()
            for j in [j for g in parts for j in range(groups[g][0], sum(groups[g]))]:
                first_sum = sums_row(j)
                carry = table[num_tm - 1, j, 1]
                for t in range(num_tm - 2, -1, -1):
                    sums[0] += table[t, j, first_sum] * carry
                    sums[1] += carry * (2.0 * table[t, j, first_sum + 1] + table[t, j, first_sum + 2] * carry)
                    if t:
                        carry = table[t, j, 1] + table[t, j, 0] * carry
        for t in range(num_tm):
            for k in range(2):
                sums[k] += table[t, last, 2 + k]
        for k in range(2):
            stats_ref[k * num_env:(k + 1) * num_env, :] = sums[k]

    for herald, devices in zip(heralds, told):
        @pl.when(here(herald))
        def _(herald=herald, devices=devices):
            listeners = [d for d in devices if d not in roots]
            for k in range(2):
                part = stats_ref[k * num_env:(k + 1) * num_env, :]
                news[k:k + 1, :] = jnp.sum(part, axis=0, keepdims=True)
            with scope("newsend"):
                for t, e in listeners:
                    if e == 0 or e == herald[1]:
                        news_copy(t, e).start()

                def tell(k, state):
                    e = jnp.where(k < herald[1], k, k + 1)
                    for t in sorted({t for t, _ in devices}):
                        news_copy(t, e).start()
                    return state

                lax.fori_loop(1, num_env - 1, tell, 0)
            with scope("newsw"):
                pending(link_sem.at[0], 2 * len(listeners)).wait_send()

    @pl.when(jnp.logical_not(is_root))
    def _():
        stats_ref[...] = jnp.zeros(stats_ref.shape, jnp.float32)
        with scope("newsr"):
            pending(root_sem.at[0], 2).wait_recv()
        for k in range(2):
            stats_ref[k * num_env:k * num_env + 1, :] = news[k:k + 1, :]


def write_kernel(cells, *refs):
    pl.run_scoped(functools.partial(write, cells, *refs), pltpu.SemaphoreType.DMA((2,)))


def write(cells, adv_ref, ret_ref, stats_ref, norm_hbm, ret_hbm, norm, sem):
    seg_rows = norm_hbm.shape[1]
    chunks = adv_ref.shape[0]
    pitch = seg_rows + PAD

    def out_copy(j, src, hbm, k):
        return pltpu.make_async_copy(
            src.at[j].reshape(SEGMENTS, pitch, LANES).at[:, pl.ds(0, seg_rows), :],
            hbm.at[:, :, pl.ds(j * LANES, LANES)],
            sem.at[k],
        )

    for j in range(chunks):
        out_copy(j, ret_ref, ret_hbm, 1).start()
    half = stats_ref.shape[0] // 2
    sums = [jnp.sum(stats_ref[k * half:(k + 1) * half, :], axis=0, keepdims=True) for k in range(2)]
    mean, square = (jnp.sum(part, axis=1, keepdims=True) * (1.0 / cells) for part in sums)
    scale = lax.rsqrt(square - mean * mean + 1.0)
    mean = jnp.broadcast_to(mean, (8, LANES))
    scale = jnp.broadcast_to(scale, (8, LANES))
    for j in range(chunks):
        for s in range(SEGMENTS):
            for r in range(0, seg_rows, 8):
                at = pl.ds(s * pitch + r, 8)
                norm[j, at, :] = (adv_ref[j, at, :] - mean) * scale
        out_copy(j, norm, norm_hbm, 0).start()
    pltpu.make_async_copy(ret_hbm, ret_hbm, sem.at[1]).wait()
    pltpu.make_async_copy(norm_hbm, norm_hbm, sem.at[0]).wait()


def local(num_tm, num_env, rewards, values, done_flags, bootstrap, discount_horizon, trace_horizon):
    steps, width = rewards.shape
    seg_rows, chunks = steps // SEGMENTS, width // LANES
    pitch = seg_rows + PAD
    split = lambda x: x.reshape(SEGMENTS, seg_rows, width)
    row = lambda x: x.reshape(1, width)
    padded = (chunks, SEGMENTS * pitch, LANES)
    tiles = (chunks, seg_rows, SEGMENTS, LANES)
    hbm = pl.BlockSpec(memory_space=pltpu.HBM)
    vmem = pl.BlockSpec(memory_space=pltpu.VMEM)
    f32 = jnp.float32
    handed = 4 * (2 * chunks * SEGMENTS * pitch + 2 * num_env) * LANES
    adv, ret, stats = pl.pallas_call(
        functools.partial(exchange_kernel, num_tm, num_env),
        out_shape=(pltpu.VMEM(padded, f32), pltpu.VMEM(padded, f32), pltpu.VMEM((2 * num_env, LANES), f32)),
        in_specs=[hbm] * 6,
        out_specs=(vmem, vmem, vmem),
        scratch_shapes=[
            pltpu.VMEM(tiles, f32),
            pltpu.VMEM(tiles, f32),
            pltpu.VMEM(tiles, jnp.int32),
            pltpu.VMEM((3, 1, width), f32),
            pltpu.VMEM(tiles, f32),
            pltpu.VMEM(tiles, f32),
            pltpu.VMEM((chunks, 8, LANES), f32),
            pltpu.VMEM((num_tm, chunks, 8, LANES), f32),
            pltpu.VMEM((num_tm, chunks, ROWS, num_env, LANES), f32),
            pltpu.VMEM((8, LANES), f32),
            pltpu.SemaphoreType.DMA((1,)),
            pltpu.SemaphoreType.DMA((2,)),
        ],
        compiler_params=pltpu.CompilerParams(collective_id=0, has_side_effects=True, vmem_limit_bytes=VMEM_BYTES - handed),
    )(split(rewards), split(values), split(done_flags), row(bootstrap), row(discount_horizon), row(trace_horizon))
    norm_advantage, return_target = pl.pallas_call(
        functools.partial(write_kernel, float(steps * width * num_tm * num_env)),
        out_shape=(jax.ShapeDtypeStruct((SEGMENTS, seg_rows, width), f32),) * 2,
        in_specs=[vmem] * 3,
        out_specs=(hbm, hbm),
        scratch_shapes=[pltpu.VMEM(padded, f32)],
        compiler_params=pltpu.CompilerParams(vmem_limit_bytes=8 * 2**20),
    )(*(pltpu.with_memory_space_constraint(x, pltpu.VMEM) for x in (adv, ret, stats)))
    return norm_advantage.reshape(steps, width), return_target.reshape(steps, width)


def solution(mesh):
    placed = (P("tm", "env"), P("tm", "env"), P("tm", "env"), P("env"), P("env"), P("env"))
    return jax.shard_map(
        functools.partial(local, mesh.shape["tm"], mesh.shape["env"]),
        mesh=mesh,
        in_specs=placed,
        out_specs=(P("tm", "env"), P("tm", "env")),
        check_vma=False,
    )
```

```python
import functools

import jax
import jax.numpy as jnp
from jax import lax
from jax.experimental import pallas as pl
from jax.experimental.pallas import tpu as pltpu
from jax.sharding import PartitionSpec as P

MESH = pl.DeviceIdType.MESH
SEGMENTS = 8
LANES = 128
PAD = 8
STEPS_UNROLLED = 64
VMEM_BYTES = 67043328
ROWS = 7
scope = jax.named_scope


def shifted(x, distance, fill):
    rows = lax.broadcasted_iota(jnp.int32, x.shape, 0)
    moved = pltpu.roll(x, SEGMENTS - distance, 0)
    return jnp.where(rows < SEGMENTS - distance, moved, fill)


def load_pieces(chunks):
    return [1] * chunks


def send_groups(chunks):
    cuts = sorted({0, max(chunks - 2, 0), chunks - 1})
    return tuple((a, b - a) for a, b in zip(cuts, cuts[1:] + [chunks]))


def exchange_kernel(
    num_tm, num_env,
    rewards_hbm, values_hbm, flags_hbm, boot_hbm, disc_hbm, trace_hbm,
    adv_ref, ret_ref, stats_ref,
    rew, val, flg, params, base, prop, out, links, table, news,
    link_sem, root_sem,
):
    me = lax.axis_index("tm")
    my_env = lax.axis_index("env")
    seg_rows, width = rewards_hbm.shape[1], rewards_hbm.shape[2]
    chunks = width // LANES
    pitch = seg_rows + PAD
    groups = send_groups(chunks)
    last = chunks - 1
    pair = 2 if num_tm % 2 == 0 else 1
    others = num_tm * num_env - 1

    silent = [(t, 0) for t in range(pair)]
    middle = num_env // 2 - 1
    heralds = [(num_tm - 1, middle), (pair - 1, middle)]
    if num_tm == pair:
        heralds = heralds[1:]
    roots = silent + heralds
    told = [
        [(t, e) for e in range(num_env) for t in range(pair, num_tm)],
        [(t, e) for e in range(1, num_env) for t in range(pair)],
    ][-len(heralds):]

    def here(device):
        return jnp.logical_and(me == device[0], my_env == device[1])

    is_root = functools.reduce(jnp.logical_or, [here(r) for r in roots])
    serves = [me >= pair, me < pair][-len(heralds):]

    def at(device):
        return {"tm": device[0], "env": device[1]}

    def rows_of(ref, n):
        count = 1
        for d in ref.shape[:-1]:
            count *= d
        return ref.reshape(count, LANES).at[pl.ds(0, n)]

    def pending(sem, n, ref=base):
        part = rows_of(ref, n)
        return pltpu.make_async_remote_copy(
            src_ref=part, dst_ref=part, send_sem=sem, recv_sem=sem,
            device_id={"tm": lax.rem(me + 1, num_tm)}, device_id_type=MESH,
        )

    def sums_row(j):
        return 4 if j == chunks - 1 else 2

    def role_of(t):
        return 2 if t == num_tm - 1 else min(t, 1)

    def span(role, g):
        after = sums_row(groups[g][0] + groups[g][1] - 1)
        return ((2, after + 1), (0, after + 3), (1, after - 1))[role]

    def sent(role, g):
        return groups[g][1] * span(role, g)[1]

    roles = [me == 0, jnp.logical_and(me > 0, me < num_tm - 1), me == num_tm - 1]

    link_rows = 2 * chunks * (num_tm - 1)

    def scan_and_send(load_sem):
        pieces = load_pieces(chunks)
        at_piece = [sum(pieces[:j]) for j in range(chunks)]

        def load(j):
            size = seg_rows // pieces[j]
            for h in range(pieces[j]):
                rows = pl.ds((pieces[j] - 1 - h) * size, size)
                for s in range(SEGMENTS):
                    for hbm, vmem in ((rewards_hbm, rew), (values_hbm, val), (flags_hbm, flg)):
                        pltpu.make_async_copy(
                            hbm.at[s, rows, pl.ds(j * LANES, LANES)], vmem.at[j, rows, s], load_sem.at[at_piece[j] + h]
                        ).start()

        load(0)
        for a, hbm in enumerate((boot_hbm, disc_hbm, trace_hbm)):
            pltpu.make_async_copy(hbm, params.at[a], load_sem.at[0]).start()
        for j in range(1, chunks):
            load(j)
        barrier = pltpu.get_barrier_semaphore()
        for k in range(1, num_tm):
            pl.semaphore_signal(barrier, inc=1, device_id={"tm": lax.rem(me + k, num_tm)}, device_id_type=MESH)

        for herald, mine in zip(heralds, serves):
            @pl.when(functools.reduce(jnp.logical_and, [my_env != herald[1], mine, jnp.logical_not(is_root)]))
            def _(herald=herald):
                pl.semaphore_signal(barrier, inc=1, device_id=at(herald), device_id_type=MESH)


        @pl.when(is_root)
        def _():
            def greet(k, state):
                for t in range(num_tm):
                    pl.semaphore_signal(
                        barrier, inc=1, device_id=at((t, lax.rem(my_env + k, num_env))), device_id_type=MESH
                    )
                return state

            lax.fori_loop(1, num_env, greet, 0)

        def link_copy(peer):
            return pltpu.make_async_remote_copy(
                src_ref=out.at[:, pl.ds(0, 2)], dst_ref=links.at[me, :, pl.ds(0, 2)],
                send_sem=load_sem.at[0], recv_sem=link_sem.at[0],
                device_id={"tm": peer}, device_id_type=MESH,
            )

        def root_copy(root, role, g):
            first, count = groups[g]
            rows = pl.ds(*span(role, g))
            return pltpu.make_async_remote_copy(
                src_ref=out.at[pl.ds(first, count), rows],
                dst_ref=table.at[me, pl.ds(first, count), rows, my_env],
                send_sem=load_sem.at[0], recv_sem=root_sem.at[0 if g < len(groups) - 1 else 1],
                device_id=at(root), device_id_type=MESH,
            )

        peers = [lax.rem(me + k, num_tm) for k in range(1, num_tm)]

        def send_block(devices, parts):
            for role in range(3):
                @pl.when(roles[role])
                def _(role=role):
                    for root in devices:
                        if role_of(root[0]) != role:
                            for g in parts:
                                root_copy(root, role, g).start()
                        else:
                            @pl.when(jnp.logical_not(here(root)))
                            def _(root=root):
                                for g in parts:
                                    root_copy(root, role, g).start()

        with scope("ldw00"):
            pending(load_sem.at[0], 3 * chunks + 3 * (seg_rows // pieces[0]) * SEGMENTS).wait_recv()
        inv_trace = 1.0 / (1.0 - 1.0 / params[2])
        discount = 1.0 - 1.0 / params[1]
        rate_all = discount * (1.0 - 1.0 / params[2])
        top = me == num_tm - 1
        ends = jnp.where(top, params[0] * inv_trace, 0.0)
        open_end = jnp.where(top, 0.0, 1.0)

        own = []
        early = max(chunks - 2, 0)
        zero = jnp.zeros((SEGMENTS, LANES), jnp.float32)
        total, squares = zero, zero
        for j in range(chunks):
            spread = lambda x: jnp.broadcast_to(x[:, j * LANES:(j + 1) * LANES], zero.shape)
            disc, rate, itr, end = spread(discount), spread(rate_all), spread(inv_trace), spread(ends)

            def steps(i, state, last_row, j=j, disc=disc, rate=rate):
                b, p, nv, s1, s2, s3, s4, s5 = state
                for u in range(min(STEPS_UNROLLED, size)):
                    r = last_row - (i * STEPS_UNROLLED + u)
                    v = val[j, r]
                    live = flg[j, r] == 0
                    d = jnp.where(live, disc, 0.0)
                    g = jnp.where(live, rate, 0.0)
                    b = (rew[j, r] - v + d * nv) + g * b
                    p = g * p
                    nv = v
                    base[j, r] = b
                    prop[j, r] = p
                    s1, s2, s3, s4, s5 = s1 + b, s2 + p, s3 + b * b, s4 + b * p, s5 + p * p
                return b, p, nv, s1, s2, s3, s4, s5

            state = (zero, zero + 1.0, zero) + (zero,) * 5
            size = seg_rows // pieces[j]
            for h in range(pieces[j]):
                if j == early and h == 0:
                    with scope("barw"):
                        far = sum(jnp.where(my_env == env, 0, 1) for _, env in roots)
                        for herald, devices in zip(heralds, told):
                            answers = sum(d[1] != herald[1] and d not in roots for d in devices)
                            far += jnp.where(here(herald), answers, 0)
                        pl.semaphore_wait(barrier, num_tm - 1 + far)
                    if len(groups) > 2:
                        with scope("send0"):
                            send_block(silent, [0])
                if j == last and h == pieces[j] - 1 and len(groups) > 2:
                    with scope("sendm"):
                        send_block(silent[:1], [1])
                if j + h:
                    with scope(f"ldw{j}{h}"):
                        pending(load_sem.at[at_piece[j] + h], 3 * size * SEGMENTS).wait_recv()
                with scope(f"scan{j}{h}"):
                    scan = functools.partial(steps, last_row=seg_rows - 1 - h * size)
                    state = lax.fori_loop(0, max(size // STEPS_UNROLLED, 1), scan, state)
            b, p, v, s1, s2, s3, s4, s5 = state
            x, a = b + v * itr, p
            for d in (1, 2, 4):
                x_next, a_next = shifted(x, d, 0.0), shifted(a, d, 1.0)
                x, a = x + a * x_next, a * a_next
            y, z = shifted(x, 1, 0.0), shifted(a, 1, 1.0)
            y, z = y + z * end, z * open_end
            own.append((y, z))
            total += s1 + s2 * y
            squares += s3 + y * (2.0 * s4 + s5 * y)
            out[j, 0:1, :] = a[0:1]
            out[j, 1:2, :] = x[0:1] + a[0:1] * end[0:1]
            for k, part in enumerate((s2 * z, (s4 + s5 * y) * z, s5 * z * z)):
                out[j, sums_row(j) + k:sums_row(j) + k + 1, :] = jnp.sum(part, axis=0, keepdims=True)
            if j == last:
                out[j, 2:3, :] = jnp.sum(total, axis=0, keepdims=True)
                out[j, 3:4, :] = jnp.sum(squares, axis=0, keepdims=True)
        with scope("send1"):
            late = range(1 if len(groups) > 2 else 0, len(groups))
            send_block(silent[:1], late[1:] if len(groups) > 2 else late)
            send_block(silent[1:], late)
        with scope("send2"):
            send_block(heralds, range(len(groups)))
            for peer in peers:
                link_copy(peer).start()

        with scope("linkw"):
            pending(link_sem.at[0], 2 * chunks * (num_tm - 1)).wait_recv()

        for j in range(chunks):
            y, z = own[j]
            carry = jnp.zeros((1, LANES), jnp.float32)
            mine = carry
            for t in range(num_tm - 1, 0, -1):
                carry = links[t, j, 1:2, :] + links[t, j, 0:1, :] * carry if t < num_tm - 1 else links[t, j, 1:2, :]
                mine = jnp.where(me == t - 1, carry, mine)
            c = y + z * jnp.where(top, 0.0, mine)

            def finish(i, state, j=j, c=c):
                for u in range(STEPS_UNROLLED):
                    r = i * STEPS_UNROLLED + u
                    rows = pl.ds(r, SEGMENTS, stride=pitch)
                    adv = base[j, r] + prop[j, r] * c
                    adv_ref[j, rows, :] = adv
                    ret_ref[j, rows, :] = adv + val[j, r]
                return state

            with scope(f"fin{j}"):
                lax.fori_loop(0, seg_rows // STEPS_UNROLLED, finish, 0)

        with scope("sendw"):
            for role in range(3):
                block = sum(sent(role, g) for g in range(len(groups)))

                @pl.when(jnp.logical_and(roles[role], is_root))
                def _(block=block):
                    pending(load_sem.at[0], link_rows + (len(roots) - 1) * block).wait_send()

                @pl.when(jnp.logical_and(roles[role], jnp.logical_not(is_root)))
                def _(block=block):
                    pending(load_sem.at[0], link_rows + len(roots) * block).wait_send()

    pl.run_scoped(scan_and_send, pltpu.SemaphoreType.DMA((sum(load_pieces(chunks)),)))

    def news_copy(t, e):
        return pltpu.make_async_remote_copy(
            src_ref=news.at[pl.ds(0, 2)], dst_ref=news.at[pl.ds(0, 2)],
            send_sem=link_sem.at[0], recv_sem=root_sem.at[0],
            device_id=at((t, e)), device_id_type=MESH,
        )

    @pl.when(is_root)
    def _():
        for j in range(chunks):
            for r in range(sums_row(j) + 3):
                table[me, j, r, pl.ds(my_env, 1), :] = out[j, r:r + 1, :]
        sums = [jnp.zeros((num_env, LANES), jnp.float32)] * 2
        for stage, parts in enumerate((range(len(groups) - 1), [len(groups) - 1])):
            with scope(f"rootw{stage}"):
                due = [sum(sent(role, g) for g in parts) for role in range(3)]
                everyone = num_env * sum(due[role_of(t)] for t in range(num_tm))
                for role in sorted({role_of(root[0]) for root in roots}):
                    if everyone:
                        @pl.when(roles[role])
                        def _(role=role):
                            pending(root_sem.at[stage], everyone - due[role], table).wait_recv()
            for j in [j for g in parts for j in range(groups[g][0], sum(groups[g]))]:
                first_sum = sums_row(j)
                carry = table[num_tm - 1, j, 1]
                for t in range(num_tm - 2, -1, -1):
                    sums[0] += table[t, j, first_sum] * carry
                    sums[1] += carry * (2.0 * table[t, j, first_sum + 1] + table[t, j, first_sum + 2] * carry)
                    if t:
                        carry = table[t, j, 1] + table[t, j, 0] * carry
        for t in range(num_tm):
            for k in range(2):
                sums[k] += table[t, last, 2 + k]
        for k in range(2):
            stats_ref[k * num_env:(k + 1) * num_env, :] = sums[k]

    for herald, devices in zip(heralds, told):
        @pl.when(here(herald))
        def _(herald=herald, devices=devices):
            listeners = [d for d in devices if d not in roots]
            for k in range(2):
                part = stats_ref[k * num_env:(k + 1) * num_env, :]
                news[k:k + 1, :] = jnp.sum(part, axis=0, keepdims=True)
            with scope("newsend"):
                for t, e in listeners:
                    if e == 0 or e == herald[1]:
                        news_copy(t, e).start()

                def tell(k, state):
                    e = jnp.where(k < herald[1], k, k + 1)
                    for t in sorted({t for t, _ in devices}):
                        news_copy(t, e).start()
                    return state

                lax.fori_loop(1, num_env - 1, tell, 0)
            with scope("newsw"):
                pending(link_sem.at[0], 2 * len(listeners)).wait_send()

    @pl.when(jnp.logical_not(is_root))
    def _():
        stats_ref[...] = jnp.zeros(stats_ref.shape, jnp.float32)
        with scope("newsr"):
            pending(root_sem.at[0], 2).wait_recv()
        for k in range(2):
            stats_ref[k * num_env:k * num_env + 1, :] = news[k:k + 1, :]


def write_kernel(cells, *refs):
    pl.run_scoped(functools.partial(write, cells, *refs), pltpu.SemaphoreType.DMA((2,)))


def write(cells, adv_ref, ret_ref, stats_ref, norm_hbm, ret_hbm, norm, sem):
    seg_rows = norm_hbm.shape[1]
    chunks = adv_ref.shape[0]
    pitch = seg_rows + PAD

    def out_copy(j, src, hbm, k):
        return pltpu.make_async_copy(
            src.at[j].reshape(SEGMENTS, pitch, LANES).at[:, pl.ds(0, seg_rows), :],
            hbm.at[:, :, pl.ds(j * LANES, LANES)],
            sem.at[k],
        )

    for j in range(chunks):
        out_copy(j, ret_ref, ret_hbm, 1).start()
    half = stats_ref.shape[0] // 2
    sums = [jnp.sum(stats_ref[k * half:(k + 1) * half, :], axis=0, keepdims=True) for k in range(2)]
    mean, square = (jnp.sum(part, axis=1, keepdims=True) * (1.0 / cells) for part in sums)
    scale = lax.rsqrt(square - mean * mean + 1.0)
    mean = jnp.broadcast_to(mean, (8, LANES))
    scale = jnp.broadcast_to(scale, (8, LANES))
    for j in range(chunks):
        for s in range(SEGMENTS):
            for r in range(0, seg_rows, 8):
                at = pl.ds(s * pitch + r, 8)
                norm[j, at, :] = (adv_ref[j, at, :] - mean) * scale
        out_copy(j, norm, norm_hbm, 0).start()
    pltpu.make_async_copy(ret_hbm, ret_hbm, sem.at[1]).wait()
    pltpu.make_async_copy(norm_hbm, norm_hbm, sem.at[0]).wait()


def local(num_tm, num_env, rewards, values, done_flags, bootstrap, discount_horizon, trace_horizon):
    steps, width = rewards.shape
    seg_rows, chunks = steps // SEGMENTS, width // LANES
    pitch = seg_rows + PAD
    split = lambda x: x.reshape(SEGMENTS, seg_rows, width)
    row = lambda x: x.reshape(1, width)
    padded = (chunks, SEGMENTS * pitch, LANES)
    tiles = (chunks, seg_rows, SEGMENTS, LANES)
    hbm = pl.BlockSpec(memory_space=pltpu.HBM)
    vmem = pl.BlockSpec(memory_space=pltpu.VMEM)
    f32 = jnp.float32
    handed = 4 * (2 * chunks * SEGMENTS * pitch + 2 * num_env) * LANES
    adv, ret, stats = pl.pallas_call(
        functools.partial(exchange_kernel, num_tm, num_env),
        out_shape=(pltpu.VMEM(padded, f32), pltpu.VMEM(padded, f32), pltpu.VMEM((2 * num_env, LANES), f32)),
        in_specs=[hbm] * 6,
        out_specs=(vmem, vmem, vmem),
        scratch_shapes=[
            pltpu.VMEM(tiles, f32),
            pltpu.VMEM(tiles, f32),
            pltpu.VMEM(tiles, jnp.int32),
            pltpu.VMEM((3, 1, width), f32),
            pltpu.VMEM(tiles, f32),
            pltpu.VMEM(tiles, f32),
            pltpu.VMEM((chunks, 8, LANES), f32),
            pltpu.VMEM((num_tm, chunks, 8, LANES), f32),
            pltpu.VMEM((num_tm, chunks, ROWS, num_env, LANES), f32),
            pltpu.VMEM((8, LANES), f32),
            pltpu.SemaphoreType.DMA((1,)),
            pltpu.SemaphoreType.DMA((2,)),
        ],
        compiler_params=pltpu.CompilerParams(collective_id=0, has_side_effects=True, vmem_limit_bytes=VMEM_BYTES - handed),
    )(split(rewards), split(values), split(done_flags), row(bootstrap), row(discount_horizon), row(trace_horizon))
    norm_advantage, return_target = pl.pallas_call(
        functools.partial(write_kernel, float(steps * width * num_tm * num_env)),
        out_shape=(jax.ShapeDtypeStruct((SEGMENTS, seg_rows, width), f32),) * 2,
        in_specs=[vmem] * 3,
        out_specs=(hbm, hbm),
        scratch_shapes=[pltpu.VMEM(padded, f32)],
        compiler_params=pltpu.CompilerParams(vmem_limit_bytes=8 * 2**20),
    )(*(pltpu.with_memory_space_constraint(x, pltpu.VMEM) for x in (adv, ret, stats)))
    return norm_advantage.reshape(steps, width), return_target.reshape(steps, width)


def solution(mesh):
    placed = (P("tm", "env"), P("tm", "env"), P("tm", "env"), P("env"), P("env"), P("env"))
    return jax.shard_map(
        functools.partial(local, mesh.shape["tm"], mesh.shape["env"]),
        mesh=mesh,
        in_specs=placed,
        out_specs=(P("tm", "env"), P("tm", "env")),
        check_vma=False,
    )
```
